512 devices in a mesh: pop: 16 (over y, core), shard: 32 (over z, x).
Axes of the slice: x: 4, y: 8, z: 8, core: 2. Of those that a mesh axis runs over, the one named last changes fastest.
Arguments:
- tokens: bfloat16 [4096, 2048], P('shard'), may hold values from -6 to 6
- targets: bfloat16 [4096, 2048], P('shard'), may hold values from -6 to 6
- norm_gain: float32 [2048], replicated, may hold values from 0.5 to 1.5
- weights: float32 [16, 2, 2048, 256], P('pop', None, 'shard'), may hold values from -6 to 6
- first_moment: float32 [16, 2, 2048, 256], P('pop', None, 'shard'), may hold values from -4 to 4
- second_moment: float32 [16, 2, 2048, 256], P('pop', None, 'shard'), may hold values from 0.05 to 2
- learned_params: float32 [192], replicated, may hold values from -4 to 4
- perturbation: float32 [8, 192], replicated, may hold values from -0.75 to 0.75
- accumulated: float32 [8, 192], replicated, may hold values from -3 to 3
Outputs:
- new_weights: float32 [16, 2, 2048, 256], P('pop', None, 'shard')
- new_first: float32 [16, 2, 2048, 256], P('pop', None, 'shard')
- new_second: float32 [16, 2, 2048, 256], P('pop', None, 'shard')
- unroll_loss: float32 [16], P('pop')
- outer_grad: float32 [192], replicated
The draws below stay inside these ranges and needn't reach their ends.
All inputs are finite; a program needn't handle non-finite values.
Results may differ from the reference program's by a relative error of at most 0.004.
Values may be sent and summed in bfloat16 or wider, within the bound.
No kernel may reach another device: no remote copies, remote signals or barrier semaphores. Data moves between devices by JAX's collectives and lax.ppermute only.
A program may use at most 64 MiB of HBM per device.

```python
import math
import jax
import jax.numpy as jnp
from jax import lax

D = 2048
RANK = 256
STEPS = 1
TOK_DEV = 128
LOPT = 192
PARTICLES = 16
PAIRS = 8
TOKENS = 4096
N_SHARD = 32


def steps_of(own_key, shape, shards, least, largest):
    loudness, own = 1.0, jax.random.fold_in(own_key, 6)
    for axis_at, blocks in shards:
        heights = jnp.exp(jax.random.uniform(jax.random.fold_in(own, axis_at), (blocks,), jnp.float32, least / len(shards), largest / len(shards)))
        loudness = loudness * jnp.repeat(heights, shape[axis_at] // blocks).reshape([-1 if axis == axis_at else 1 for axis in range(len(shape))])
    return loudness


def centred(rng, extent, scale, bound, split=(), kind=jnp.bfloat16):
    entries = jax.random.normal(rng, extent, jnp.float32) * scale
    if len(split) > 0:
        entries = steps_of(rng, extent, split, -0.22, 0.18) * entries
    return jnp.clip(entries, min=-bound, max=bound).astype(kind)


def setup_inputs(seed: int = 0) -> dict:
    key_list = jax.random.split(jax.random.key(seed), 10)
    return {
        "tokens": centred(key_list[0], (TOKENS, D), 1.0, 6.0, ((0, 32),)),
        "targets": centred(key_list[1], (TOKENS, D), 1.0, 6.0, ((0, 32),)),
        "norm_gain": jnp.clip(1.0 + 0.1 * jax.random.normal(key_list[2], (D,), jnp.float32), 0.5, 1.5),
        "weights": centred(key_list[3], (PARTICLES, 2, D, RANK), 1.0, 6.0, ((0, 16), (2, 32)), jnp.float32),
        "first_moment": centred(key_list[4], (PARTICLES, 2, D, RANK), 0.3, 4.0, ((0, 16), (2, 32)), jnp.float32),
        "second_moment": jnp.clip(jnp.exp(math.log(2.0) - 3.6888794 * jax.random.uniform(key_list[5], (PARTICLES, 2, D, RANK), jnp.float32) ** steps_of(key_list[5], (PARTICLES, 2, D, RANK), ((0, 16), (2, 32)), -0.2, 0.2)), 0.05, 2.0),
        "learned_params": centred(key_list[6], (LOPT,), 0.5, 4.0, (), jnp.float32),
        "perturbation": centred(key_list[7], (PAIRS, LOPT), 0.05, 0.75, (), jnp.float32),
        "accumulated": centred(key_list[8], (PAIRS, LOPT), 0.2, 3.0, (), jnp.float32),
    }


step_size = 0.1
beta_one = 0.9
beta_two = 0.99
norm_eps = 1e-05
grad_eps = 1e-06

def learned_update(weights, first_state, second_state, gradient, mean_square, learned):
    hidden_units = learned.shape[0] // 6
    scaled = gradient * lax.rsqrt(mean_square + grad_eps)[:, None, None]
    first_new = beta_one * first_state + (1.0 - beta_one) * scaled
    second_new = beta_two * second_state + (1.0 - beta_two) * scaled * scaled
    inverse = lax.rsqrt(second_new)
    momentum = (first_new * inverse).reshape(-1)
    features = jnp.stack([(scaled * inverse).reshape(-1), momentum, weights.reshape(-1)])
    in_map = learned[:3 * hidden_units].reshape(3, hidden_units)
    in_bias = learned[3 * hidden_units:4 * hidden_units]
    out_map = learned[4 * hidden_units:].reshape(2, hidden_units)
    hidden_act = jnp.tanh(jnp.dot(in_map.T, features, precision=lax.Precision.HIGHEST) + in_bias[:, None])
    outputs = jnp.dot(out_map, hidden_act, precision=lax.Precision.HIGHEST)
    change = -step_size * (momentum + outputs[0]) * jnp.exp(jnp.tanh(outputs[1]))
    return (weights + change.reshape(weights.shape), first_new, second_new)

def normalize(tokens, norm_gain):
    values = tokens.astype(jnp.float32)
    inverse = lax.rsqrt(lax.optimization_barrier(jnp.mean(values * values, axis=-1, keepdims=True)) + norm_eps)
    return (values * inverse * norm_gain).astype(jnp.bfloat16)

def block_sum(normed_blocks, right_blocks, factor):
    parts = jnp.einsum('jtd,jtr->jdr', normed_blocks.astype(jnp.float32), right_blocks.astype(jnp.float32)) * factor
    rounded = lax.optimization_barrier(parts.astype(jnp.bfloat16))
    return lax.optimization_barrier(jnp.sum(rounded.astype(jnp.float32), axis=0))

def reference(tokens, targets, norm_gain, weights, first_moment, second_moment, learned_params, perturbation, accumulated):
    normed = normalize(tokens, norm_gain)
    tokens_wide = tokens.astype(jnp.float32)
    target_wide = targets.astype(jnp.float32)
    down_scale = D ** (-0.5)
    up_scale = RANK ** (-0.5)

    def particle(inputs):
        particle_index, current, first_state, second_state = inputs
        polarity = (1 - 2 * (particle_index % 2)).astype(jnp.float32)
        learned = learned_params + polarity * perturbation[particle_index // 2]
        running_loss = jnp.zeros((), jnp.float32)
        for unroll_step in range(STEPS):
            rounded = current.astype(jnp.bfloat16)
            branch_input = jnp.dot(normed, rounded[0], preferred_element_type=jnp.float32) * down_scale
            active = jax.nn.silu(branch_input).astype(jnp.bfloat16)
            branch = lax.dot_general(active, rounded[1], (((1,), (1,)), ((), ())), preferred_element_type=jnp.float32) * up_scale
            residual = tokens_wide + branch - target_wide
            running_loss = running_loss + jnp.sum(residual * residual) / (TOKENS * D)
            upstream = (2.0 * residual).astype(jnp.bfloat16)
            back_act = jnp.dot(upstream, rounded[1], preferred_element_type=jnp.float32) * up_scale
            logistic = jax.nn.sigmoid(branch_input)
            back = (back_act * logistic * (1.0 + branch_input * (1.0 - logistic))).astype(jnp.bfloat16)
            grad_down = block_sum(normed.reshape(N_SHARD, TOK_DEV, D), back.reshape(N_SHARD, TOK_DEV, RANK), down_scale)
            grad_up = block_sum(upstream.reshape(N_SHARD, TOK_DEV, D), active.reshape(N_SHARD, TOK_DEV, RANK), up_scale)
            gradient = jnp.stack([grad_down, grad_up])
            mean_square = lax.optimization_barrier(jnp.mean(gradient * gradient, axis=(1, 2)))
            current, first_state, second_state = learned_update(current, first_state, second_state, gradient, mean_square, learned)
        return (current, first_state, second_state, running_loss)
    indices = jnp.arange(PARTICLES, dtype=jnp.int32)
    new_weights, new_first, new_second, unroll_loss = lax.map(particle, (indices, weights, first_moment, second_moment))
    pair_diff = unroll_loss[0::2] - unroll_loss[1::2]
    outer_grad = jnp.dot(pair_diff, accumulated + perturbation, precision=lax.Precision.HIGHEST) / (2 * PAIRS)
    return (new_weights, new_first, new_second, unroll_loss, outer_grad)
```

```python
import jax
import jax.numpy as jnp
from jax import lax
from jax.sharding import Mesh, PartitionSpec as P

D = 2048
RANK = 256

step_size = 0.1
beta_one = 0.9
beta_two = 0.99
norm_eps = 1e-05
grad_eps = 1e-06
f32 = jnp.float32
bf16 = jnp.bfloat16


def from_everyone(array, axis):
    copies = jnp.broadcast_to(array, (lax.axis_size(axis), *array.shape))
    return lax.all_to_all(copies, axis, split_axis=0, concat_axis=0, tiled=True)


def learned_update(weights, first_state, second_state, gradient, mean_square, learned):
    hidden_units = learned.shape[0] // 6
    scaled = gradient * lax.rsqrt(mean_square + grad_eps)[:, None, None]
    first_new = beta_one * first_state + (1.0 - beta_one) * scaled
    second_new = beta_two * second_state + (1.0 - beta_two) * scaled * scaled
    inverse = lax.rsqrt(second_new)
    momentum = (first_new * inverse).reshape(-1)
    features = jnp.stack([(scaled * inverse).reshape(-1), momentum, weights.reshape(-1)])
    in_map = learned[: 3 * hidden_units].reshape(3, hidden_units)
    in_bias = learned[3 * hidden_units : 4 * hidden_units]
    out_map = learned[4 * hidden_units :].reshape(2, hidden_units)
    hidden_act = jnp.tanh(jnp.dot(in_map.T, features) + in_bias[:, None])
    outputs = jnp.dot(out_map, hidden_act)
    change = -step_size * (momentum + outputs[0]) * jnp.exp(jnp.tanh(outputs[1]))
    return (weights + change.reshape(weights.shape), first_new, second_new)


def normalize(tokens, norm_gain):
    values = tokens.astype(f32)
    inverse = lax.rsqrt(jnp.mean(values * values, axis=-1, keepdims=True) + norm_eps)
    return (values * inverse * norm_gain).astype(bf16)


def shift(array, axis, step):
    count = lax.axis_size(axis)
    return lax.ppermute(array, axis, [(i, (i + step) % count) for i in range(count)])


def swap(array, axis, mask):
    return lax.ppermute(array, axis, [(i, i ^ mask) for i in range(lax.axis_size(axis))])


def local(
    tokens,
    targets,
    norm_gain,
    weights,
    first_moment,
    second_moment,
    learned_params,
    perturbation,
    accumulated,
):
    nz, nx = lax.axis_size("z"), lax.axis_size("x")
    particles = lax.axis_size("y") * lax.axis_size("core")
    my_x = lax.axis_index("x")
    rows = weights.shape[2]
    block = tokens.shape[0]
    width = nz * rows
    total_tokens = block * nz * nx
    down_scale = D ** (-0.5)
    up_scale = RANK ** (-0.5)
    particle = lax.axis_index("y") * lax.axis_size("core") + lax.axis_index("core")
    polarity = (1 - 2 * (particle % 2)).astype(f32)
    pair_index = particle // 2
    learned = learned_params + polarity * lax.dynamic_index_in_dim(
        perturbation, pair_index, 0, keepdims=False
    )

    gathered = from_everyone(weights[0].astype(bf16), "z")
    down_w = gathered[:, 0].reshape(width, RANK)
    up_w = gathered[:, 1].reshape(width, RANK)

    normed = normalize(tokens, norm_gain)
    cut = jnp.stack([normed, tokens, targets]).reshape(3, block, nz, nx, rows)
    cut = jnp.transpose(cut, (3, 0, 1, 2, 4)).reshape(nx, 3, block, width)

    def slot(array, step):
        return lax.dynamic_index_in_dim(array, (my_x + step) % nx, 0, keepdims=False)

    parts = [slot(cut, 0)] + [shift(slot(cut, k), "x", k) for k in range(1, nx)]
    normed_x, tokens_x, targets_x = (
        jnp.concatenate([p[i] for p in parts], axis=0) for i in range(3)
    )

    def summed_over_x(partial):
        blocks = partial.astype(bf16)
        total = partial
        for k in range(1, nx):
            turned = jnp.roll(blocks, k * block, axis=0)
            total = total + shift(turned, "x", k).astype(f32)
        return total

    branch_input = summed_over_x(
        jnp.dot(normed_x, down_w, preferred_element_type=f32) * down_scale
    )
    active = jax.nn.silu(branch_input).astype(bf16)
    branch = (
        lax.dot_general(active, up_w, (((1,), (1,)), ((), ())), preferred_element_type=f32)
        * up_scale
    )
    residual = tokens_x.astype(f32) + branch - targets_x.astype(f32)
    loss_part = jnp.sum(residual * residual)
    upstream = (2.0 * residual).astype(bf16)
    back_act = summed_over_x(jnp.dot(upstream, up_w, preferred_element_type=f32) * up_scale)
    logistic = jax.nn.sigmoid(branch_input)
    back = (back_act * logistic * (1.0 + branch_input * (1.0 - logistic))).astype(bf16)
    down_term = (
        lax.dot_general(normed_x, back, (((0,), (0,)), ((), ())), preferred_element_type=f32)
        * down_scale
    )
    up_term = (
        lax.dot_general(upstream, active, (((0,), (0,)), ((), ())), preferred_element_type=f32)
        * up_scale
    )
    terms = jnp.stack(
        [
            down_term.astype(bf16).reshape(nz, rows, RANK),
            up_term.astype(bf16).reshape(nz, rows, RANK),
        ],
        axis=1,
    )
    gradient = jnp.sum(
        lax.all_to_all(terms, "z", 0, 0, tiled=True).astype(f32), axis=0
    )

    losses = jnp.where(jnp.arange(particles) == particle, loss_part, 0.0)
    losses = losses + swap(losses, "core", 1)
    for mask in (1, 2, 4):
        losses = losses + swap(losses, "y", mask)
    squares = jnp.sum(gradient * gradient, axis=(1, 2))
    sums = jnp.sum(from_everyone(jnp.concatenate([squares, losses]), ("z", "x")), axis=0)
    mean_square = sums[:2] / (D * RANK)
    all_losses = sums[2:] / (total_tokens * D)

    current, first_state, second_state = learned_update(
        weights[0], first_moment[0], second_moment[0], gradient, mean_square, learned
    )
    own_loss = lax.dynamic_index_in_dim(all_losses, particle, 0, keepdims=True)
    pair_diff = all_losses[0::2] - all_losses[1::2]
    outer_grad = jnp.sum(pair_diff[:, None] * (accumulated + perturbation), axis=0) / particles
    return (current[None], first_state[None], second_state[None], own_loss, outer_grad)


def solution(mesh):
    grid = Mesh(mesh.devices.reshape(8, 2, 8, 4), ("y", "core", "z", "x"))
    pop, shard = ("y", "core"), ("z", "x")
    return jax.shard_map(
        local,
        mesh=grid,
        in_specs=(
            P(shard, None),
            P(shard, None),
            P(),
            P(pop, None, shard, None),
            P(pop, None, shard, None),
            P(pop, None, shard, None),
            P(),
            P(),
            P(),
        ),
        out_specs=(
            P(pop, None, shard, None),
            P(pop, None, shard, None),
            P(pop, None, shard, None),
            P(pop),
            P(),
        ),
        check_vma=False,
    )
```

```python
import jax
import jax.numpy as jnp
from jax import lax
from jax.experimental import pallas as pl
from jax.experimental.pallas import tpu as pltpu
from jax.sharding import Mesh, PartitionSpec as P

D = 2048
RANK = 256
HIDDEN = 32

step_size = 0.1
beta_one = 0.9
beta_two = 0.99
norm_eps = 1e-05
grad_eps = 1e-06
down_scale = D ** (-0.5)
up_scale = RANK ** (-0.5)
f32 = jnp.float32
bf16 = jnp.bfloat16
VMEM = pl.BlockSpec(memory_space=pltpu.VMEM)
SMEM = pl.BlockSpec(memory_space=pltpu.SMEM)


def call(kernel, outs, args, flops, name):
    scalars = [a.dtype == jnp.int32 or a.ndim == 1 for a in args]
    moved = sum(a.size * a.dtype.itemsize for a in args)
    return pl.pallas_call(
        kernel,
        out_shape=[jax.ShapeDtypeStruct(s, d) for s, d in outs],
        in_specs=[SMEM if s else VMEM for s in scalars],
        out_specs=[VMEM] * len(outs),
        compiler_params=pltpu.CompilerParams(vmem_limit_bytes=16 * 2**20),
        cost_estimate=pl.CostEstimate(flops=flops, bytes_accessed=moved, transcendentals=0),
        name=name,
    )(*args)


def cut_kernel(place, tokens, targets, gain, *outs):
    block, rows = tokens.shape[0], 64
    lanes = lax.broadcasted_iota(jnp.int32, (block, 128), 1) < rows
    values = tokens[...].astype(f32)
    inverse = lax.rsqrt(jnp.mean(values * values, axis=-1, keepdims=True) + norm_eps)
    for k in range(4):
        x = lax.rem(place[0] + k, 4)
        high, odd = x // 2, lax.rem(x, 2) == 1
        keep = jnp.logical_xor(lanes, odd)
        for q in range(4):
            spots = [pl.ds(pl.multiple_of((2 * q + j) * 256 + high * 128, 128), 128) for j in range(2)]

            def merged(pair):
                a, b = pair
                return jnp.where(
                    keep, jnp.where(odd, b, a), pltpu.roll(jnp.where(odd, a, b), rows, 1)
                )

            out = pl.ds(q * 128, 128)
            toks = [tokens[:, s].astype(f32) for s in spots]
            norms = [t * inverse * gain[:, s] for t, s in zip(toks, spots)]
            outs[k][:, out] = merged(norms).astype(bf16)
            outs[4 + k][0:block, out] = merged(toks).astype(bf16)
            outs[4 + k][block : 2 * block, out] = merged(
                [targets[:, s].astype(f32) for s in spots]
            ).astype(bf16)


def spread(parts, own, sends):
    count = len(parts)
    for i, part in enumerate(parts):
        height = part.shape[0]
        own[i * height : (i + 1) * height, :] = part
        small = part.astype(bf16)
        for k in range(1, count):
            j = (i + k) % count
            sends[k - 1][j * height : (j + 1) * height, :] = small


def first_kernel(n0, n1, n2, n3, gathered, own, s1, s2, s3):
    down_w = gathered[:, 0].reshape(-1, RANK)
    parts = [
        jnp.dot(n[...], down_w, preferred_element_type=f32) * down_scale for n in (n0, n1, n2, n3)
    ]
    spread(parts, own, (s1, s2, s3))


def middle_kernel(
    own, r1, r2, r3, t0, t1, t2, t3, gathered, slope, active_out, upstream_out, loss, back, s1, s2, s3
):
    up_w = gathered[:, 1].reshape(-1, RANK)
    parts, losses = [], 0.0
    for i, t in enumerate((t0, t1, t2, t3)):
        block = t.shape[0] // 2
        at = pl.ds(i * block, block)
        pre = (own[at, :] + r1[at, :].astype(f32)) + (r2[at, :].astype(f32) + r3[at, :].astype(f32))
        logistic = jax.nn.sigmoid(pre)
        slope[at, :] = logistic * (1.0 + pre * (1.0 - logistic))
        active = (pre * logistic).astype(bf16)
        active_out[at, :] = active
        branch = lax.dot_general(
            active, up_w, (((1,), (1,)), ((), ())), preferred_element_type=f32
        )
        residual = (
            t[0:block, :].astype(f32) + branch * up_scale - t[block : 2 * block, :].astype(f32)
        )
        losses = losses + jnp.sum(residual * residual, axis=0, keepdims=True)
        upstream = (2.0 * residual).astype(bf16)
        upstream_out[at, :] = upstream
        parts.append(jnp.dot(upstream, up_w, preferred_element_type=f32) * up_scale)
    loss[...] = losses
    spread(parts, back, (s1, s2, s3))


def last_kernel(own, r1, r2, r3, slope, n0, n1, n2, n3, upstream, active, terms):
    count, _, rows, _ = terms.shape
    total = (own[...] + r1[...].astype(f32)) + (r2[...].astype(f32) + r3[...].astype(f32))
    back = (total * slope[...]).astype(bf16)
    turned = (((0,), (0,)), ((), ()))
    up = lax.dot_general(upstream[...], active[...], turned, preferred_element_type=f32) * up_scale
    terms[:, 1] = up.astype(bf16).reshape(count, rows, RANK)
    down = 0.0
    for i, n in enumerate((n0, n1, n2, n3)):
        block = n.shape[0]
        down = down + lax.dot_general(
            n[...], back[i * block : (i + 1) * block], turned, preferred_element_type=f32
        )
    terms[:, 0] = (down * down_scale).astype(bf16).reshape(count, rows, RANK)


def update_kernel(
    number,
    learned,
    sums,
    gradient,
    weights,
    first,
    second,
    accumulated,
    perturbation,
    new_weights,
    new_first,
    new_second,
    own_loss,
    outer,
):
    total = jnp.sum(sums[...], axis=0, keepdims=True)
    lane = lax.broadcasted_iota(jnp.int32, total.shape, 1)
    elements = weights.shape[0] * weights.shape[1] * weights.shape[2] * sums.shape[0] // 2
    pairs = accumulated.shape[0]
    own_loss[...] = jnp.sum(jnp.where(lane == 2 + number[0], total, 0.0), axis=1, keepdims=True)
    row = lax.broadcasted_iota(jnp.int32, (pairs, total.shape[1]), 0)
    spot = lax.broadcasted_iota(jnp.int32, (pairs, total.shape[1]), 1)
    signs = jnp.where(spot == 2 + 2 * row, 1.0, 0.0) - jnp.where(spot == 3 + 2 * row, 1.0, 0.0)
    difference = jnp.sum(signs * total, axis=1, keepdims=True)
    outer[...] = jnp.sum(
        difference * (accumulated[...] + perturbation[...]), axis=0, keepdims=True
    ) / (2 * pairs)
    chunk = 32
    for half in range(2):
        square = jnp.sum(jnp.where(lane == half, total, 0.0), axis=1, keepdims=True)
        factor = lax.rsqrt(square / elements + grad_eps)
        for start in range(0, weights.shape[1], chunk):
            at = (half, pl.ds(start, chunk))
            weight = weights[at]
            scaled = gradient[at] * factor
            m = beta_one * first[at] + (1.0 - beta_one) * scaled
            v = beta_two * second[at] + (1.0 - beta_two) * scaled * scaled
            new_first[at] = m
            new_second[at] = v
            inverse = lax.rsqrt(v)
            momentum = m * inverse
            speed = scaled * inverse
            out_a = jnp.zeros_like(momentum)
            out_b = jnp.zeros_like(momentum)
            for h in range(HIDDEN):
                act = jnp.tanh(
                    speed * learned[h]
                    + momentum * learned[HIDDEN + h]
                    + weight * learned[2 * HIDDEN + h]
                    + learned[3 * HIDDEN + h]
                )
                out_a = out_a + act * learned[4 * HIDDEN + h]
                out_b = out_b + act * learned[5 * HIDDEN + h]
            new_weights[at] = weight - step_size * (momentum + out_a) * jnp.exp(jnp.tanh(out_b))


def from_everyone(array, axis):
    copies = jnp.broadcast_to(array, (lax.axis_size(axis), *array.shape))
    return lax.all_to_all(copies, axis, split_axis=0, concat_axis=0, tiled=True)


def shift(array, axis, step):
    count = lax.axis_size(axis)
    return lax.ppermute(array, axis, [(i, (i + step) % count) for i in range(count)])


def local(
    tokens,
    targets,
    norm_gain,
    weights,
    first_moment,
    second_moment,
    learned_params,
    perturbation,
    accumulated,
):
    nz, nx = lax.axis_size("z"), lax.axis_size("x")
    particles = lax.axis_size("y") * lax.axis_size("core")
    rows = weights.shape[2]
    block = tokens.shape[0]
    width = nz * rows
    tall = nx * block
    total_tokens = tall * nz
    particle = lax.axis_index("y") * lax.axis_size("core") + lax.axis_index("core")
    polarity = (1 - 2 * (particle % 2)).astype(f32)
    learned = learned_params + polarity * lax.dynamic_index_in_dim(
        perturbation, particle // 2, 0, keepdims=False
    )

    gathered = from_everyone(weights[0].astype(bf16), "z")
    place = lax.axis_index("x").astype(jnp.int32)[None]
    pieces = call(
        cut_kernel,
        [((block, width), bf16)] * 4 + [((2 * block, width), bf16)] * 4,
        (place, tokens, targets, norm_gain[None]),
        20 * block * D,
        "cut",
    )
    normed = [pieces[0]] + [shift(pieces[k], "x", k) for k in range(1, nx)]
    pairs = [pieces[4]] + [shift(pieces[4 + k], "x", k) for k in range(1, nx)]

    wide, thin = ((tall, RANK), f32), ((tall, RANK), bf16)
    product = 2 * tall * width * RANK
    pre, *sends = call(first_kernel, [wide] + [thin] * 3, (*normed, gathered), product, "first")
    sends = [shift(s, "x", k + 1) for k, s in enumerate(sends)]
    slope, active, upstream, loss, back, *sends = call(
        middle_kernel,
        [wide, thin, ((tall, width), bf16), ((1, width), f32), wide] + [thin] * 3,
        (pre, *sends, *pairs, gathered),
        2 * product,
        "middle",
    )
    sends = [shift(s, "x", k + 1) for k, s in enumerate(sends)]
    shares = from_everyone(jnp.sum(loss)[None, None], ("y", "core"))
    sends, shares = lax.optimization_barrier((sends, shares))
    (terms,) = call(
        last_kernel,
        [((nz, 2, rows, RANK), bf16)],
        (back, *sends, slope, *normed, upstream, active),
        2 * product,
        "last",
    )
    gradient = jnp.sum(lax.all_to_all(terms, "z", 0, 0, tiled=True).astype(f32), axis=0)
    squares = jnp.sum(gradient * gradient, axis=(1, 2))
    line = jnp.concatenate([squares, shares.reshape(-1) / (total_tokens * D)])
    line = jnp.pad(line, (0, 128 - line.shape[0]))
    sums = from_everyone(line, ("z", "x"))
    shape = (weights.shape[1], rows, RANK)
    new_w, new_m, new_v, own_loss, outer = call(
        update_kernel,
        [(shape, f32)] * 3 + [((1, 1), f32), ((1, learned.shape[0]), f32)],
        (
            particle.astype(jnp.int32)[None],
            learned,
            sums,
            gradient,
            weights[0],
            first_moment[0],
            second_moment[0],
            accumulated,
            perturbation,
        ),
        400 * weights.size,
        "update",
    )
    return (new_w[None], new_m[None], new_v[None], own_loss.reshape(1), outer.reshape(-1))


def solution(mesh):
    grid = Mesh(mesh.devices.reshape(8, 2, 8, 4), ("y", "core", "z", "x"))
    pop, shard = ("y", "core"), ("z", "x")
    return jax.shard_map(
        local,
        mesh=grid,
        in_specs=(
            P(shard, None),
            P(shard, None),
            P(),
            P(pop, None, shard, None),
            P(pop, None, shard, None),
            P(pop, None, shard, None),
            P(),
            P(),
            P(),
        ),
        out_specs=(
            P(pop, None, shard, None),
            P(pop, None, shard, None),
            P(pop, None, shard, None),
            P(pop),
            P(),
        ),
        check_vma=False,
    )
```

```python
import jax
import jax.numpy as jnp
from jax import lax
from jax.experimental import pallas as pl
from jax.experimental.pallas import tpu as pltpu
from jax.sharding import Mesh, PartitionSpec as P

D = 2048
RANK = 256
HIDDEN = 32

step_size = 0.1
beta_one = 0.9
beta_two = 0.99
norm_eps = 1e-05
grad_eps = 1e-06
down_scale = D ** (-0.5)
up_scale = RANK ** (-0.5)
f32 = jnp.float32
bf16 = jnp.bfloat16
VMEM = pl.BlockSpec(memory_space=pltpu.VMEM)
SMEM = pl.BlockSpec(memory_space=pltpu.SMEM)


def call(kernel, outs, args, flops, name):
    scalars = [a.ndim == 1 for a in args]
    moved = sum(a.size * a.dtype.itemsize for a in args)
    return pl.pallas_call(
        kernel,
        out_shape=[jax.ShapeDtypeStruct(s, d) for s, d in outs],
        in_specs=[SMEM if s else VMEM for s in scalars],
        out_specs=[VMEM] * len(outs),
        compiler_params=pltpu.CompilerParams(vmem_limit_bytes=16 * 2**20),
        cost_estimate=pl.CostEstimate(flops=flops, bytes_accessed=moved, transcendentals=0),
        name=name,
    )(*args)


def copies_kernel(weights, copies):
    for i in range(copies.shape[0]):
        copies[i] = weights[...].astype(bf16)


def cut_kernel(tokens, targets, gain, *outs):
    block, rows = tokens.shape[0], 64
    lanes = lax.broadcasted_iota(jnp.int32, (block, 128), 1) < rows
    my_x = lax.axis_index("x")
    values = tokens[...].astype(f32)
    inverse = lax.rsqrt(jnp.mean(values * values, axis=-1, keepdims=True) + norm_eps)
    for k, dest in enumerate(outs):
        x = jnp.bitwise_xor(my_x, k)
        high, odd = x // 2, lax.rem(x, 2) == 1
        keep = jnp.logical_xor(lanes, odd)
        for q in range(4):
            spots = [pl.ds(pl.multiple_of((2 * q + j) * 256 + high * 128, 128), 128) for j in range(2)]

            def merged(pair):
                a, b = pair
                return jnp.where(
                    keep, jnp.where(odd, b, a), pltpu.roll(jnp.where(odd, a, b), rows, 1)
                )

            out = pl.ds(q * 128, 128)
            toks = [tokens[:, s].astype(f32) for s in spots]
            norms = [t * inverse * gain[:, s] for t, s in zip(toks, spots)]
            gaps = [t - targets[:, s].astype(f32) for t, s in zip(toks, spots)]
            dest[0:block, out] = merged(norms).astype(bf16)
            dest[block : 2 * block, out] = merged(gaps).astype(bf16)


def particle_index():
    return lax.axis_index("y") * lax.axis_size("core") + lax.axis_index("core")


def spread(parts, own, sends):
    count = len(parts)
    for i, part in enumerate(parts):
        height = part.shape[0]
        own[i * height : (i + 1) * height, :] = part
        small = part.astype(bf16)
        for k in range(1, count):
            j = i ^ k
            sends[k - 1][j * height : (j + 1) * height, :] = small


def first_kernel(n0, n1, n2, n3, gathered, own, s1, s2, s3):
    down_w = gathered[:, 0].reshape(-1, RANK)
    block = n0.shape[0] // 2
    parts = [
        jnp.dot(n[0:block, :], down_w, preferred_element_type=f32) * down_scale
        for n in (n0, n1, n2, n3)
    ]
    spread(parts, own, (s1, s2, s3))


def middle_kernel(
    own, r1, r2, r3, t0, t1, t2, t3, gathered, slope, active_out, upstream_out, loss, back, s1, s2, s3
):
    up_w = gathered[:, 1].reshape(-1, RANK)
    parts, losses = [], 0.0
    for i, t in enumerate((t0, t1, t2, t3)):
        block = t.shape[0] // 2
        at = pl.ds(i * block, block)
        pre = (own[at, :] + r1[at, :].astype(f32)) + (r2[at, :].astype(f32) + r3[at, :].astype(f32))
        logistic = jax.nn.sigmoid(pre)
        slope[at, :] = logistic * (1.0 + pre * (1.0 - logistic))
        active = (pre * logistic).astype(bf16)
        active_out[at, :] = active
        branch = lax.dot_general(
            active, up_w, (((1,), (1,)), ((), ())), preferred_element_type=f32
        )
        residual = t[block : 2 * block, :].astype(f32) + branch * up_scale
        losses = losses + jnp.sum(residual * residual, axis=0, keepdims=True)
        upstream = (2.0 * residual).astype(bf16)
        upstream_out[at, :] = upstream
        parts.append(jnp.dot(upstream, up_w, preferred_element_type=f32) * up_scale)
    lane = lax.broadcasted_iota(jnp.int32, loss.shape, 1)
    mean = jnp.sum(losses, axis=1, keepdims=True) / (own.shape[0] * lax.axis_size("z") * D)
    loss[...] = jnp.where(lane == 2 + particle_index(), mean, 0.0)
    spread(parts, back, (s1, s2, s3))


def last_kernel(own, r1, r2, r3, slope, n0, n1, n2, n3, upstream, active, terms):
    count, _, rows, _ = terms.shape
    total = (own[...] + r1[...].astype(f32)) + (r2[...].astype(f32) + r3[...].astype(f32))
    back = (total * slope[...]).astype(bf16)
    turned = (((0,), (0,)), ((), ()))
    up = lax.dot_general(upstream[...], active[...], turned, preferred_element_type=f32) * up_scale
    terms[:, 1] = up.astype(bf16).reshape(count, rows, RANK)
    down = 0.0
    for i, n in enumerate((n0, n1, n2, n3)):
        block = n.shape[0] // 2
        down = down + lax.dot_general(
            n[0:block, :], back[i * block : (i + 1) * block], turned, preferred_element_type=f32
        )
    terms[:, 0] = (down * down_scale).astype(bf16).reshape(count, rows, RANK)


def total_kernel(received, losses, gradient, line):
    lane = lax.broadcasted_iota(jnp.int32, losses.shape, 1)
    full = losses[...]
    for half in range(gradient.shape[0]):
        total = received[0, half].astype(f32)
        for i in range(1, received.shape[0]):
            total = total + received[i, half].astype(f32)
        gradient[half] = total
        square = jnp.sum(jnp.sum(total * total, axis=0, keepdims=True), axis=1, keepdims=True)
        full = full + jnp.where(lane == half, square, 0.0)
    line[...] = jnp.broadcast_to(full[None], line.shape)


def add_kernel(a, b, out):
    out[...] = a[...] + b[...]


def learned_kernel(base, perturbation, out):
    particle = particle_index()
    row = lax.broadcasted_iota(jnp.int32, perturbation.shape, 0)
    own = jnp.sum(
        jnp.where(row == particle // 2, perturbation[...], 0.0), axis=0, keepdims=True
    )
    out[...] = base[...] + jnp.where(lax.rem(particle, 2) == 0, own, -own)


def update_kernel(
    learned,
    sums,
    gradient,
    weights,
    first,
    second,
    accumulated,
    perturbation,
    new_weights,
    new_first,
    new_second,
    own_loss,
    outer,
):
    total = jnp.sum(sums[...], axis=0)
    lane = lax.broadcasted_iota(jnp.int32, total.shape, 1)
    elements = weights.shape[0] * weights.shape[1] * weights.shape[2] * sums.shape[0] // 2
    pairs = accumulated.shape[0]
    own_loss[...] = jnp.sum(jnp.where(lane == 2 + particle_index(), total, 0.0), axis=1, keepdims=True)
    row = lax.broadcasted_iota(jnp.int32, (pairs, total.shape[1]), 0)
    spot = lax.broadcasted_iota(jnp.int32, (pairs, total.shape[1]), 1)
    signs = jnp.where(spot == 2 + 2 * row, 1.0, 0.0) - jnp.where(spot == 3 + 2 * row, 1.0, 0.0)
    difference = jnp.sum(signs * total, axis=1, keepdims=True)
    outer[...] = jnp.sum(
        difference * (accumulated[...] + perturbation[...]), axis=0, keepdims=True
    ) / (2 * pairs)
    chunk = 32
    for half in range(2):
        square = jnp.sum(jnp.where(lane == half, total, 0.0), axis=1, keepdims=True)
        factor = lax.rsqrt(square / elements + grad_eps)
        for start in range(0, weights.shape[1], chunk):
            at = (half, pl.ds(start, chunk))
            weight = weights[at]
            scaled = gradient[at] * factor
            m = beta_one * first[at] + (1.0 - beta_one) * scaled
            v = beta_two * second[at] + (1.0 - beta_two) * scaled * scaled
            new_first[at] = m
            new_second[at] = v
            inverse = lax.rsqrt(v)
            momentum = m * inverse
            speed = scaled * inverse
            out_a = jnp.zeros_like(momentum)
            out_b = jnp.zeros_like(momentum)
            for h in range(HIDDEN):
                act = jnp.tanh(
                    speed * learned[h]
                    + momentum * learned[HIDDEN + h]
                    + weight * learned[2 * HIDDEN + h]
                    + learned[3 * HIDDEN + h]
                )
                out_a = out_a + act * learned[4 * HIDDEN + h]
                out_b = out_b + act * learned[5 * HIDDEN + h]
            new_weights[at] = weight - step_size * (momentum + out_a) * jnp.exp(jnp.tanh(out_b))


def swap(array, axis, mask):
    return lax.ppermute(array, axis, [(i, i ^ mask) for i in range(lax.axis_size(axis))])


def plus(a, b):
    return call(add_kernel, [(a.shape, a.dtype)], (a, b), a.size, "plus")[0]


def local(
    tokens,
    targets,
    norm_gain,
    weights,
    first_moment,
    second_moment,
    learned_params,
    perturbation,
    accumulated,
):
    nz, nx = lax.axis_size("z"), lax.axis_size("x")
    rows = weights.shape[2]
    block = tokens.shape[0]
    width = nz * rows
    tall = nx * block
    shape = (weights.shape[1], rows, RANK)
    (copies,) = call(copies_kernel, [((nz, *shape), bf16)], (weights[0],), weights.size, "copies")
    gathered = lax.all_to_all(copies, "z", 0, 0, tiled=True)
    pieces = call(
        cut_kernel,
        [((2 * block, width), bf16)] * nx,
        (tokens, targets, norm_gain[None]),
        20 * block * D,
        "cut",
    )
    pieces = [pieces[0]] + [swap(pieces[k], "x", k) for k in range(1, nx)]

    wide, thin = ((tall, RANK), f32), ((tall, RANK), bf16)
    product = 2 * tall * width * RANK
    pre, *sends = call(first_kernel, [wide] + [thin] * 3, (*pieces, gathered), product, "first")
    sends = [swap(s, "x", k + 1) for k, s in enumerate(sends)]
    slope, active, upstream, loss, back, *sends = call(
        middle_kernel,
        [wide, thin, ((tall, width), bf16), ((1, 128), f32), wide] + [thin] * 3,
        (pre, *sends, *pieces, gathered),
        2 * product,
        "middle",
    )
    sends = [swap(s, "x", k + 1) for k, s in enumerate(sends)]
    loss = plus(loss, swap(loss, "core", 1))
    loss = plus(loss, swap(loss, "y", 1))
    sends, loss = lax.optimization_barrier((sends, loss))
    (terms,) = call(
        last_kernel,
        [((nz, *shape), bf16)],
        (back, *sends, slope, *pieces, upstream, active),
        2 * product,
        "last",
    )
    terms = lax.all_to_all(terms, "z", 0, 0, tiled=True)
    loss = plus(loss, swap(loss, "y", 2))
    loss = plus(loss, swap(loss, "y", 4))
    gradient, line = call(
        total_kernel,
        [(shape, f32), ((nz * nx, 1, 128), f32)],
        (terms, loss),
        10 * terms.size,
        "total",
    )
    sums = lax.all_to_all(line, ("z", "x"), 0, 0, tiled=True)
    (learned,) = call(
        learned_kernel,
        [((1, learned_params.shape[0]), f32)],
        (learned_params[None], perturbation),
        10 * perturbation.size,
        "learned",
    )
    learned = learned.reshape(-1)
    new_w, new_m, new_v, own_loss, outer = call(
        update_kernel,
        [(shape, f32)] * 3 + [((1, 1), f32), ((1, learned.shape[0]), f32)],
        (
            learned,
            sums,
            gradient,
            weights[0],
            first_moment[0],
            second_moment[0],
            accumulated,
            perturbation,
        ),
        400 * weights.size,
        "update",
    )
    return (new_w[None], new_m[None], new_v[None], own_loss.reshape(1), outer.reshape(-1))


def solution(mesh):
    grid = Mesh(mesh.devices.reshape(8, 2, 8, 4), ("y", "core", "z", "x"))
    pop, shard = ("y", "core"), ("z", "x")
    return jax.shard_map(
        local,
        mesh=grid,
        in_specs=(
            P(shard, None),
            P(shard, None),
            P(),
            P(pop, None, shard, None),
            P(pop, None, shard, None),
            P(pop, None, shard, None),
            P(),
            P(),
            P(),
        ),
        out_specs=(
            P(pop, None, shard, None),
            P(pop, None, shard, None),
            P(pop, None, shard, None),
            P(pop),
            P(),
        ),
        check_vma=False,
    )
```

```python
import jax
import jax.numpy as jnp
from jax import lax
from jax.experimental import pallas as pl
from jax.experimental.pallas import tpu as pltpu
from jax.sharding import Mesh, PartitionSpec as P

D = 2048
RANK = 256
HIDDEN = 32

step_size = 0.1
beta_one = 0.9
beta_two = 0.99
norm_eps = 1e-05
grad_eps = 1e-06
down_scale = D ** (-0.5)
up_scale = RANK ** (-0.5)
f32 = jnp.float32
bf16 = jnp.bfloat16
VMEM = pl.BlockSpec(memory_space=pltpu.VMEM)
SMEM = pl.BlockSpec(memory_space=pltpu.SMEM)


def call(kernel, outs, args, flops, name, scratch=()):
    scalars = [a.ndim == 1 for a in args]
    moved = sum(a.size * a.dtype.itemsize for a in args)
    return pl.pallas_call(
        kernel,
        out_shape=[jax.ShapeDtypeStruct(s, d) for s, d in outs],
        in_specs=[SMEM if s else VMEM for s in scalars],
        out_specs=[VMEM] * len(outs),
        scratch_shapes=[pltpu.VMEM(s, d) for s, d in scratch],
        compiler_params=pltpu.CompilerParams(vmem_limit_bytes=16 * 2**20),
        cost_estimate=pl.CostEstimate(flops=flops, bytes_accessed=moved, transcendentals=0),
        name=name,
    )(*args)


def copies_kernel(weights, copies):
    for i in range(copies.shape[0]):
        copies[i] = weights[...].astype(bf16)


def cut_kernel(tokens, targets, gain, *outs):
    block, tile = tokens.shape[0], 128
    my_x = lax.axis_index("x")
    outer = my_x // 2 == lax.rem(my_x, 2)
    lanes = lax.broadcasted_iota(jnp.int32, (block, tile), 1) < tile // 2
    values = tokens[...].astype(f32)
    inverse = lax.rsqrt(jnp.mean(values * values, axis=-1, keepdims=True) + norm_eps)
    for q in range(tokens.shape[1] // (2 * tile)):
        norms, gaps = [], []
        for j in range(2):
            at = slice((2 * q + j) * tile, (2 * q + j + 1) * tile)
            token = tokens[:, at].astype(f32)
            norms.append((token * inverse * gain[:, at]).astype(bf16).astype(f32))
            gaps.append(token - targets[:, at].astype(f32))
        out = slice(q * tile, (q + 1) * tile)
        for k, dest in enumerate(outs):
            first = jnp.logical_xor(lanes, outer if k else jnp.logical_not(outer))
            dest[0:block, out] = jnp.where(first, *norms).astype(bf16)
            dest[block : 2 * block, out] = jnp.where(first, *gaps).astype(bf16)


def split_kernel(gathered, down_w, up_w):
    down_w[...] = gathered[:, 0]
    up_w[...] = gathered[:, 1]


def halves():
    half = lax.rem(lax.axis_index("x"), 2)
    rows = 64
    return [pl.ds(pl.multiple_of(h * rows, rows), rows) for h in (half, 1 - half)]


def particle_index():
    return lax.axis_index("y") * lax.axis_size("core") + lax.axis_index("core")


def joined(mine, theirs, full):
    own, other = halves()
    full[:, own] = mine[...]
    full[:, other] = theirs[...]
    return full[...].reshape(-1, full.shape[-1])


def first_kernel(n0, n1, mine, theirs, own, send, full):
    down_w = joined(mine, theirs, full)
    block = n0.shape[0] // 2
    for i, n in enumerate((n0, n1)):
        part = jnp.dot(n[0:block, :], down_w, preferred_element_type=f32) * down_scale
        own[i * block : (i + 1) * block, :] = part
        send[(1 - i) * block : (2 - i) * block, :] = part.astype(bf16)


def middle_kernel(
    own, received, d0, d1, mine, theirs, slope, active_out, upstream_out, loss, back, send, full
):
    up_w = joined(mine, theirs, full)
    losses = 0.0
    block = d0.shape[0] // 2
    for i, d in enumerate((d0, d1)):
        at = slice(i * block, (i + 1) * block)
        pre = own[at, :] + received[at, :].astype(f32)
        logistic = jax.nn.sigmoid(pre)
        slope[at, :] = logistic * (1.0 + pre * (1.0 - logistic))
        active = (pre * logistic).astype(bf16)
        active_out[at, :] = active
        branch = lax.dot_general(
            active, up_w, (((1,), (1,)), ((), ())), preferred_element_type=f32
        )
        residual = d[block : 2 * block, :].astype(f32) + branch * up_scale
        losses = losses + jnp.sum(residual * residual, axis=0, keepdims=True)
        upstream = (2.0 * residual).astype(bf16)
        upstream_out[at, :] = upstream
        part = jnp.dot(upstream, up_w, preferred_element_type=f32) * up_scale
        back[at, :] = part
        send[(1 - i) * block : (2 - i) * block, :] = part.astype(bf16)
    lane = lax.broadcasted_iota(jnp.int32, loss.shape, 1)
    tokens = own.shape[0] * (lax.axis_size("x") // 2) * lax.axis_size("z")
    mean = jnp.sum(losses, axis=1, keepdims=True) / (tokens * D)
    loss[...] = jnp.where(lane == 2 + particle_index(), mean, 0.0)


def parted(product, mine, theirs, full):
    own, other = halves()
    full[...] = product.reshape(full.shape)
    mine[...] = full[:, own]
    theirs[...] = full[:, other].astype(bf16)


def up_kernel(upstream, active, mine, theirs, full):
    turned = (((0,), (0,)), ((), ()))
    up = lax.dot_general(upstream[...], active[...], turned, preferred_element_type=f32)
    parted(up * up_scale, mine, theirs, full)


def down_kernel(own, received, slope, n0, n1, mine, theirs, full):
    back = ((own[...] + received[...].astype(f32)) * slope[...]).astype(bf16)
    down = 0.0
    for i, n in enumerate((n0, n1)):
        block = n.shape[0] // 2
        down = down + lax.dot_general(
            n[0:block, :],
            back[i * block : (i + 1) * block],
            (((0,), (0,)), ((), ())),
            preferred_element_type=f32,
        )
    parted(down * down_scale, mine, theirs, full)


def terms_kernel(down, down_in, up, up_in, terms):
    terms[:, 0] = (down[...] + down_in[...].astype(f32)).astype(bf16)
    terms[:, 1] = (up[...] + up_in[...].astype(f32)).astype(bf16)


def total_kernel(received, losses, gradient, line):
    lane = lax.broadcasted_iota(jnp.int32, losses.shape, 1)
    full = losses[...]
    for half in range(gradient.shape[0]):
        total = received[0, half].astype(f32)
        for i in range(1, received.shape[0]):
            total = total + received[i, half].astype(f32)
        gradient[half] = total
        square = jnp.sum(jnp.sum(total * total, axis=0, keepdims=True), axis=1, keepdims=True)
        full = full + jnp.where(lane == half, square, 0.0)
    line[...] = jnp.broadcast_to(full[None], line.shape)


def add_kernel(a, b, out):
    out[...] = a[...] + b[...]


def learned_kernel(base, perturbation, out):
    particle = particle_index()
    row = lax.broadcasted_iota(jnp.int32, perturbation.shape, 0)
    own = jnp.sum(
        jnp.where(row == particle // 2, perturbation[...], 0.0), axis=0, keepdims=True
    )
    out[...] = base[...] + jnp.where(lax.rem(particle, 2) == 0, own, -own)


def update_kernel(
    learned,
    sums,
    gradient,
    weights,
    first,
    second,
    accumulated,
    perturbation,
    new_weights,
    new_first,
    new_second,
    own_loss,
    outer,
):
    total = jnp.sum(sums[...], axis=0)
    lane = lax.broadcasted_iota(jnp.int32, total.shape, 1)
    elements = weights.shape[0] * weights.shape[1] * weights.shape[2] * sums.shape[0] // 2
    pairs = accumulated.shape[0]
    own_loss[...] = jnp.sum(jnp.where(lane == 2 + particle_index(), total, 0.0), axis=1, keepdims=True)
    row = lax.broadcasted_iota(jnp.int32, (pairs, total.shape[1]), 0)
    spot = lax.broadcasted_iota(jnp.int32, (pairs, total.shape[1]), 1)
    signs = jnp.where(spot == 2 + 2 * row, 1.0, 0.0) - jnp.where(spot == 3 + 2 * row, 1.0, 0.0)
    difference = jnp.sum(signs * total, axis=1, keepdims=True)
    outer[...] = jnp.sum(
        difference * (accumulated[...] + perturbation[...]), axis=0, keepdims=True
    ) / (2 * pairs)
    chunk = 32
    for half in range(2):
        square = jnp.sum(jnp.where(lane == half, total, 0.0), axis=1, keepdims=True)
        factor = lax.rsqrt(square / elements + grad_eps)
        for start in range(0, weights.shape[1], chunk):
            at = (half, pl.ds(start, chunk))
            weight = weights[at]
            scaled = gradient[at] * factor
            m = beta_one * first[at] + (1.0 - beta_one) * scaled
            v = beta_two * second[at] + (1.0 - beta_two) * scaled * scaled
            new_first[at] = m
            new_second[at] = v
            inverse = lax.rsqrt(v)
            momentum = m * inverse
            speed = scaled * inverse
            out_a = jnp.zeros_like(momentum)
            out_b = jnp.zeros_like(momentum)
            for h in range(HIDDEN):
                act = jnp.tanh(
                    speed * learned[h]
                    + momentum * learned[HIDDEN + h]
                    + weight * learned[2 * HIDDEN + h]
                    + learned[3 * HIDDEN + h]
                )
                out_a = out_a + act * learned[4 * HIDDEN + h]
                out_b = out_b + act * learned[5 * HIDDEN + h]
            new_weights[at] = weight - step_size * (momentum + out_a) * jnp.exp(jnp.tanh(out_b))


def swap(array, axis, mask):
    return lax.ppermute(array, axis, [(i, i ^ mask) for i in range(lax.axis_size(axis))])


def plus(a, b):
    return call(add_kernel, [(a.shape, a.dtype)], (a, b), a.size, "plus")[0]


def local(
    tokens,
    targets,
    norm_gain,
    weights,
    first_moment,
    second_moment,
    learned_params,
    perturbation,
    accumulated,
):
    nz, nx = lax.axis_size("z"), lax.axis_size("x")
    rows = weights.shape[2]
    block = tokens.shape[0]
    width = 2 * nz * rows
    tall = 2 * block
    shape = (weights.shape[1], rows, RANK)
    column = (nz, rows, RANK)
    full = (nz, 2 * rows, RANK)
    (copies,) = call(copies_kernel, [((nz, *shape), bf16)], (weights[0],), weights.size, "copies")
    gathered = lax.all_to_all(copies, "z", 0, 0, tiled=True)
    piece, send = call(
        cut_kernel,
        [((2 * block, width), bf16)] * 2,
        (tokens, targets, norm_gain[None]),
        20 * block * D,
        "cut",
    )
    pieces = (piece, swap(send, "x", 1))
    down_w, up_w = call(split_kernel, [(column, bf16)] * 2, (gathered,), gathered.size, "split")
    down_w, up_w = (down_w, swap(down_w, "x", 3)), (up_w, swap(up_w, "x", 3))

    wide, thin = ((tall, RANK), f32), ((tall, RANK), bf16)
    product = 2 * tall * width * RANK
    joint, sums_of = [(full, bf16)], [(full, f32)]
    pre, send = call(first_kernel, [wide, thin], (*pieces, *down_w), product, "first", joint)
    slope, active, upstream, loss, back, send = call(
        middle_kernel,
        [wide, thin, ((tall, width), bf16), ((1, 128), f32), wide, thin],
        (pre, swap(send, "x", 1), *pieces, *up_w),
        2 * product,
        "middle",
        joint,
    )
    received = swap(send, "x", 1)
    parts = [(column, f32), (column, bf16)]
    up, send_up = call(up_kernel, parts, (upstream, active), product, "up", sums_of)
    up_in = swap(send_up, "x", 3)
    loss = plus(loss, swap(loss, "core", 1))
    received, _, loss = lax.optimization_barrier((received, send_up, loss))
    down, send_down = call(
        down_kernel, parts, (back, received, slope, *pieces), product, "down", sums_of
    )
    down_in = swap(send_down, "x", 3)
    loss = plus(loss, swap(loss, "y", 1))
    down_in, loss = lax.optimization_barrier((down_in, loss))
    (terms,) = call(
        terms_kernel, [((nz, *shape), bf16)], (down, down_in, up, up_in), 4 * down.size, "terms"
    )
    terms = lax.all_to_all(terms, "z", 0, 0, tiled=True)
    loss = plus(loss, swap(loss, "y", 2))
    loss = plus(loss, swap(loss, "y", 4))
    gradient, line = call(
        total_kernel,
        [(shape, f32), ((nz * nx, 1, 128), f32)],
        (terms, loss),
        10 * terms.size,
        "total",
    )
    sums = lax.all_to_all(line, ("z", "x"), 0, 0, tiled=True)
    (learned,) = call(
        learned_kernel,
        [((1, learned_params.shape[0]), f32)],
        (learned_params[None], perturbation),
        10 * perturbation.size,
        "learned",
    )
    learned = learned.reshape(-1)
    new_w, new_m, new_v, own_loss, outer = call(
        update_kernel,
        [(shape, f32)] * 3 + [((1, 1), f32), ((1, learned.shape[0]), f32)],
        (
            learned,
            sums,
            gradient,
            weights[0],
            first_moment[0],
            second_moment[0],
            accumulated,
            perturbation,
        ),
        400 * weights.size,
        "update",
    )
    return (new_w[None], new_m[None], new_v[None], own_loss.reshape(1), outer.reshape(-1))


def solution(mesh):
    grid = Mesh(mesh.devices.reshape(8, 2, 8, 4), ("y", "core", "z", "x"))
    pop, shard = ("y", "core"), ("z", "x")
    return jax.shard_map(
        local,
        mesh=grid,
        in_specs=(
            P(shard, None),
            P(shard, None),
            P(),
            P(pop, None, shard, None),
            P(pop, None, shard, None),
            P(pop, None, shard, None),
            P(),
            P(),
            P(),
        ),
        out_specs=(
            P(pop, None, shard, None),
            P(pop, None, shard, None),
            P(pop, None, shard, None),
            P(pop),
            P(),
        ),
        check_vma=False,
    )
```

```python
import jax
import jax.numpy as jnp
from jax import lax
from jax.experimental import pallas as pl
from jax.experimental.pallas import tpu as pltpu
from jax.sharding import Mesh, PartitionSpec as P


D = 2048
RANK = 256
HIDDEN = 32

step_size = 0.1
beta_one = 0.9
beta_two = 0.99
norm_eps = 1e-05
grad_eps = 1e-06
down_scale = D ** (-0.5)
up_scale = RANK ** (-0.5)
f32 = jnp.float32
bf16 = jnp.bfloat16
VMEM = pl.BlockSpec(memory_space=pltpu.VMEM)
SMEM = pl.BlockSpec(memory_space=pltpu.SMEM)


def call(kernel, outs, args, flops, scratch=()):
    scalars = [a.ndim == 1 for a in args]
    moved = sum(a.size * a.dtype.itemsize for a in args)
    return pl.pallas_call(
        kernel,
        out_shape=[jax.ShapeDtypeStruct(s, d) for s, d in outs],
        in_specs=[SMEM if s else VMEM for s in scalars],
        out_specs=[VMEM] * len(outs),
        scratch_shapes=[pltpu.VMEM(s, d) for s, d in scratch],
        compiler_params=pltpu.CompilerParams(vmem_limit_bytes=16 * 2**20),
        cost_estimate=pl.CostEstimate(flops=flops, bytes_accessed=moved, transcendentals=0),
    )(*args)


def copies_kernel(weights, copies):
    for i in range(copies.shape[0]):
        copies[i] = weights[...].astype(bf16)


def cut_kernel(tokens, targets, gain, *outs):
    block, tile = tokens.shape[0], 128
    my_x = lax.axis_index("x")
    outer = my_x // 2 == lax.rem(my_x, 2)
    lanes = lax.broadcasted_iota(jnp.int32, (block, tile), 1) < tile // 2
    values = tokens[...].astype(f32)
    inverse = lax.rsqrt(jnp.mean(values * values, axis=-1, keepdims=True) + norm_eps)
    for q in range(tokens.shape[1] // (2 * tile)):
        norms, gaps = [], []
        for j in range(2):
            at = slice((2 * q + j) * tile, (2 * q + j + 1) * tile)
            token = tokens[:, at].astype(f32)
            norms.append((token * inverse * gain[:, at]).astype(bf16).astype(f32))
            gaps.append(token - targets[:, at].astype(f32))
        out = slice(q * tile, (q + 1) * tile)
        for k, dest in enumerate(outs):
            first = jnp.logical_xor(lanes, outer if k else jnp.logical_not(outer))
            dest[0:block, out] = jnp.where(first, *norms).astype(bf16)
            dest[block : 2 * block, out] = jnp.where(first, *gaps).astype(bf16)


def split_kernel(gathered, down_w, up_w):
    down_w[...] = gathered[:, 0]
    up_w[...] = gathered[:, 1]


def halves():
    half = lax.rem(lax.axis_index("x"), 2)
    rows = 64
    return [pl.ds(pl.multiple_of(h * rows, rows), rows) for h in (half, 1 - half)]


def particle_index():
    return lax.axis_index("y") * lax.axis_size("core") + lax.axis_index("core")


def joined(mine, theirs, full):
    own, other = halves()
    full[:, own] = mine[...]
    full[:, other] = theirs[...]
    return full[...].reshape(-1, full.shape[-1])


def first_kernel(n0, n1, mine, theirs, own, send, full):
    down_w = joined(mine, theirs, full)
    block = n0.shape[0] // 2
    for i, n in enumerate((n0, n1)):
        part = jnp.dot(n[0:block, :], down_w, preferred_element_type=f32) * down_scale
        own[i * block : (i + 1) * block, :] = part
        send[(1 - i) * block : (2 - i) * block, :] = part.astype(bf16)


def middle_kernel(
    own, received, d0, d1, mine, theirs, slope, active_out, upstream_out, loss, back, send, full
):
    up_w = joined(mine, theirs, full)
    losses = 0.0
    block = d0.shape[0] // 2
    for i, d in enumerate((d0, d1)):
        at = slice(i * block, (i + 1) * block)
        pre = own[at, :] + received[at, :].astype(f32)
        logistic = jax.nn.sigmoid(pre)
        slope[at, :] = logistic * (1.0 + pre * (1.0 - logistic))
        active = (pre * logistic).astype(bf16)
        active_out[at, :] = active
        branch = lax.dot_general(
            active, up_w, (((1,), (1,)), ((), ())), preferred_element_type=f32
        )
        residual = d[block : 2 * block, :].astype(f32) + branch * up_scale
        losses = losses + jnp.sum(residual * residual, axis=0, keepdims=True)
        upstream = (2.0 * residual).astype(bf16)
        upstream_out[at, :] = upstream
        part = jnp.dot(upstream, up_w, preferred_element_type=f32) * up_scale
        back[at, :] = part
        send[(1 - i) * block : (2 - i) * block, :] = part.astype(bf16)
    lane = lax.broadcasted_iota(jnp.int32, (1, 128), 1)
    tokens = own.shape[0] * (lax.axis_size("x") // 2) * lax.axis_size("z")
    mean = jnp.sum(losses, axis=1, keepdims=True) / (tokens * D)
    line = jnp.where(lane == 2 + particle_index(), mean, 0.0)
    loss[...] = jnp.broadcast_to(line[None], loss.shape)


def parted(product, mine, theirs, full):
    own, other = halves()
    full[...] = product.reshape(full.shape)
    mine[...] = full[:, own]
    theirs[...] = full[:, other].astype(bf16)


def up_kernel(upstream, active, mine, theirs, full):
    turned = (((0,), (0,)), ((), ()))
    up = lax.dot_general(upstream[...], active[...], turned, preferred_element_type=f32)
    parted(up * up_scale, mine, theirs, full)


def down_kernel(own, received, slope, n0, n1, mine, theirs, full):
    back = ((own[...] + received[...].astype(f32)) * slope[...]).astype(bf16)
    down = 0.0
    for i, n in enumerate((n0, n1)):
        block = n.shape[0] // 2
        down = down + lax.dot_general(
            n[0:block, :],
            back[i * block : (i + 1) * block],
            (((0,), (0,)), ((), ())),
            preferred_element_type=f32,
        )
    parted(down * down_scale, mine, theirs, full)


def terms_kernel(down, down_in, up, up_in, terms):
    terms[:, 0] = (down[...] + down_in[...].astype(f32)).astype(bf16)
    terms[:, 1] = (up[...] + up_in[...].astype(f32)).astype(bf16)


def total_kernel(received, losses, gradient, line):
    full = jnp.sum(losses[...], axis=0)
    lane = lax.broadcasted_iota(jnp.int32, full.shape, 1)
    for half in range(gradient.shape[0]):
        total = received[0, half].astype(f32)
        for i in range(1, received.shape[0]):
            total = total + received[i, half].astype(f32)
        gradient[half] = total
        square = jnp.sum(jnp.sum(total * total, axis=0, keepdims=True), axis=1, keepdims=True)
        full = full + jnp.where(lane == half, square, 0.0)
    line[...] = jnp.broadcast_to(full[None], line.shape)


def learned_kernel(base, perturbation, out):
    particle = particle_index()
    row = lax.broadcasted_iota(jnp.int32, perturbation.shape, 0)
    own = jnp.sum(
        jnp.where(row == particle // 2, perturbation[...], 0.0), axis=0, keepdims=True
    )
    out[...] = base[...] + jnp.where(lax.rem(particle, 2) == 0, own, -own)


def update_kernel(
    learned,
    sums,
    gradient,
    weights,
    first,
    second,
    accumulated,
    perturbation,
    new_weights,
    new_first,
    new_second,
    own_loss,
    outer,
):
    total = jnp.sum(sums[...], axis=0)
    lane = lax.broadcasted_iota(jnp.int32, total.shape, 1)
    elements = weights.shape[0] * weights.shape[1] * weights.shape[2] * sums.shape[0] // 2
    pairs = accumulated.shape[0]
    own_loss[...] = jnp.sum(jnp.where(lane == 2 + particle_index(), total, 0.0), axis=1, keepdims=True)
    row = lax.broadcasted_iota(jnp.int32, (pairs, total.shape[1]), 0)
    spot = lax.broadcasted_iota(jnp.int32, (pairs, total.shape[1]), 1)
    signs = jnp.where(spot == 2 + 2 * row, 1.0, 0.0) - jnp.where(spot == 3 + 2 * row, 1.0, 0.0)
    difference = jnp.sum(signs * total, axis=1, keepdims=True)
    outer[...] = jnp.sum(
        difference * (accumulated[...] + perturbation[...]), axis=0, keepdims=True
    ) / (2 * pairs)
    chunk = 32
    for half in range(2):
        square = jnp.sum(jnp.where(lane == half, total, 0.0), axis=1, keepdims=True)
        factor = lax.rsqrt(square / elements + grad_eps)
        for start in range(0, weights.shape[1], chunk):
            at = (half, pl.ds(start, chunk))
            weight = weights[at]
            scaled = gradient[at] * factor
            m = beta_one * first[at] + (1.0 - beta_one) * scaled
            v = beta_two * second[at] + (1.0 - beta_two) * scaled * scaled
            new_first[at] = m
            new_second[at] = v
            inverse = lax.rsqrt(v)
            momentum = m * inverse
            speed = scaled * inverse
            out_a = jnp.zeros_like(momentum)
            out_b = jnp.zeros_like(momentum)
            for h in range(HIDDEN):
                act = jnp.tanh(
                    speed * learned[h]
                    + momentum * learned[HIDDEN + h]
                    + weight * learned[2 * HIDDEN + h]
                    + learned[3 * HIDDEN + h]
                )
                out_a = out_a + act * learned[4 * HIDDEN + h]
                out_b = out_b + act * learned[5 * HIDDEN + h]
            new_weights[at] = weight - step_size * (momentum + out_a) * jnp.exp(jnp.tanh(out_b))


def swap(array, axis, mask):
    pairs = [(i, i ^ mask) for i in range(lax.axis_size(axis))]
    return lax.ppermute(array, axis, pairs)


def exchange(array, axis):
    return lax.all_to_all(array, axis, 0, 0, tiled=True)


def local(
    tokens,
    targets,
    norm_gain,
    weights,
    first_moment,
    second_moment,
    learned_params,
    perturbation,
    accumulated,
):
    nz, nx = lax.axis_size("z"), lax.axis_size("x")
    particles = lax.axis_size("y") * lax.axis_size("core")
    rows = weights.shape[2]
    block = tokens.shape[0]
    width = 2 * nz * rows
    tall = 2 * block
    shape = (weights.shape[1], rows, RANK)
    column = (nz, rows, RANK)
    full = (nz, 2 * rows, RANK)
    (copies,) = call(copies_kernel, [((nz, *shape), bf16)], (weights[0],), weights.size)
    gathered = exchange(copies, "z")
    piece, send = call(
        cut_kernel,
        [((2 * block, width), bf16)] * 2,
        (tokens, targets, norm_gain[None]),
        20 * block * D,
    )
    pieces = (piece, swap(send, "x", 1))
    down_w, up_w = call(split_kernel, [(column, bf16)] * 2, (gathered,), gathered.size)
    down_w, up_w = (down_w, swap(down_w, "x", 3)), (up_w, swap(up_w, "x", 3))

    wide, thin = ((tall, RANK), f32), ((tall, RANK), bf16)
    product = 2 * tall * width * RANK
    joint, sums_of = [(full, bf16)], [(full, f32)]
    pre, send = call(first_kernel, [wide, thin], (*pieces, *down_w), product, joint)
    slope, active, upstream, loss, back, send = call(
        middle_kernel,
        [wide, thin, ((tall, width), bf16), ((particles, 1, 128), f32), wide, thin],
        (pre, swap(send, "x", 1), *pieces, *up_w),
        2 * product,
        joint,
    )
    received = swap(send, "x", 1)
    parts = [(column, f32), (column, bf16)]
    up, send_up = call(up_kernel, parts, (upstream, active), product, sums_of)
    up_in = swap(send_up, "x", 3)
    down, send_down = call(down_kernel, parts, (back, received, slope, *pieces), product, sums_of)
    down_in = swap(send_down, "x", 3)
    loss = exchange(loss, ("y", "core"))
    (terms,) = call(terms_kernel, [((nz, *shape), bf16)], (down, down_in, up, up_in), 4 * down.size)
    terms = exchange(terms, "z")
    gradient, line = call(
        total_kernel, [(shape, f32), ((nz * nx, 1, 128), f32)], (terms, loss), 10 * terms.size
    )
    sums = exchange(line, ("z", "x"))
    (learned,) = call(
        learned_kernel,
        [((1, learned_params.shape[0]), f32)],
        (learned_params[None], perturbation),
        10 * perturbation.size,
    )
    learned = learned.reshape(-1)
    new_w, new_m, new_v, own_loss, outer = call(
        update_kernel,
        [(shape, f32)] * 3 + [((1, 1), f32), ((1, learned.shape[0]), f32)],
        (
            learned,
            sums,
            gradient,
            weights[0],
            first_moment[0],
            second_moment[0],
            accumulated,
            perturbation,
        ),
        400 * weights.size,
    )
    return (new_w[None], new_m[None], new_v[None], own_loss.reshape(1), outer.reshape(-1))


def solution(mesh):
    grid = Mesh(mesh.devices.reshape(8, 2, 8, 4), ("y", "core", "z", "x"))
    pop, shard = ("y", "core"), ("z", "x")
    return jax.shard_map(
        local,
        mesh=grid,
        in_specs=(
            P(shard, None),
            P(shard, None),
            P(),
            P(pop, None, shard, None),
            P(pop, None, shard, None),
            P(pop, None, shard, None),
            P(),
            P(),
            P(),
        ),
        out_specs=(
            P(pop, None, shard, None),
            P(pop, None, shard, None),
            P(pop, None, shard, None),
            P(pop),
            P(),
        ),
        check_vma=False,
    )
```

```python
import jax
import jax.numpy as jnp
from jax import lax
from jax.experimental import pallas as pl
from jax.experimental.pallas import tpu as pltpu
from jax.sharding import Mesh, PartitionSpec as P


D = 2048
RANK = 256
HIDDEN = 32

step_size = 0.1
beta_one = 0.9
beta_two = 0.99
norm_eps = 1e-05
grad_eps = 1e-06
down_scale = D ** (-0.5)
up_scale = RANK ** (-0.5)
f32 = jnp.float32
bf16 = jnp.bfloat16
VMEM = pl.BlockSpec(memory_space=pltpu.VMEM)
SMEM = pl.BlockSpec(memory_space=pltpu.SMEM)


def call(kernel, outs, args, flops, scratch=()):
    scalars = [a.ndim == 1 for a in args]
    moved = sum(a.size * a.dtype.itemsize for a in args)
    return pl.pallas_call(
        kernel,
        out_shape=[jax.ShapeDtypeStruct(s, d) for s, d in outs],
        in_specs=[SMEM if s else VMEM for s in scalars],
        out_specs=[VMEM] * len(outs),
        scratch_shapes=[pltpu.VMEM(s, d) for s, d in scratch],
        compiler_params=pltpu.CompilerParams(vmem_limit_bytes=16 * 2**20),
        cost_estimate=pl.CostEstimate(flops=flops, bytes_accessed=moved, transcendentals=0),
    )(*args)


def copies_kernel(weights, copies):
    for i in range(copies.shape[0]):
        copies[i] = weights[...].astype(bf16)


def cut_kernel(tokens, targets, gain, *outs):
    tile = 128
    block, side = tokens.shape[0], tile // 2
    my_x = lax.axis_index("x")
    outer = my_x // 2 == lax.rem(my_x, 2)
    lanes = lax.broadcasted_iota(jnp.int32, (block, tile), 1) < side
    values = tokens[...].astype(f32)
    inverse = lax.rsqrt(jnp.mean(values * values, axis=-1, keepdims=True) + norm_eps)
    norms = []
    for q in range(tokens.shape[1] // (2 * tile)):
        pair, gaps = [], []
        for j in range(2):
            at = slice((2 * q + j) * tile, (2 * q + j + 1) * tile)
            token = tokens[:, at].astype(f32)
            pair.append(token * inverse * gain[:, at])
            gaps.append(token - targets[:, at].astype(f32))
        norms.append(pair)
        out = slice(q * tile, (q + 1) * tile)
        for k, dest in enumerate(outs[4:]):
            first = jnp.logical_xor(lanes, outer if k else jnp.logical_not(outer))
            dest[:, out] = jnp.where(first, *gaps).astype(bf16)
    for k, dest in enumerate(outs[:4]):
        x = jnp.bitwise_xor(my_x, k)
        high, odd = x // 2 == 1, lax.rem(x, 2) == 1
        keep = jnp.logical_xor(lanes, odd)
        for q in range(len(norms) // 2):
            a, b = (jnp.where(high, n[1], n[0]) for n in norms[2 * q : 2 * q + 2])
            moved = pltpu.roll(jnp.where(odd, a, b), side, 1)
            kept = jnp.where(odd, b, a)
            dest[:, q * tile : (q + 1) * tile] = jnp.where(keep, kept, moved).astype(bf16)


def split_kernel(gathered, up_w):
    up_w[...] = gathered[:, 1]


def halves():
    half = lax.rem(lax.axis_index("x"), 2)
    rows = 64
    return [pl.ds(pl.multiple_of(h * rows, rows), rows) for h in (half, 1 - half)]


def particle_index():
    return lax.axis_index("y") * lax.axis_size("core") + lax.axis_index("core")


def joined(mine, theirs, full):
    own, other = halves()
    full[:, own] = mine[...]
    full[:, other] = theirs[...]
    return full[...].reshape(-1, full.shape[-1])


def first_kernel(n0, n1, n2, n3, gathered, own, s1, s2, s3):
    down_w = gathered[:, 0].reshape(-1, RANK)
    block = n0.shape[0]
    for i, n in enumerate((n0, n1, n2, n3)):
        part = jnp.dot(n[...], down_w, preferred_element_type=f32) * down_scale
        for k, dest in enumerate((own, s1, s2, s3)):
            j = i ^ k
            if j < 2:
                dest[j * block : (j + 1) * block, :] = part.astype(dest.dtype)


def middle_kernel(
    own, r1, r2, r3, d0, d1, mine, theirs, slope, active_out, upstream_out, loss, back, send, full
):
    up_w = joined(mine, theirs, full)
    losses = 0.0
    block = d0.shape[0]
    for i, d in enumerate((d0, d1)):
        at = slice(i * block, (i + 1) * block)
        pre = (own[at, :] + r1[at, :].astype(f32)) + (r2[at, :].astype(f32) + r3[at, :].astype(f32))
        logistic = jax.nn.sigmoid(pre)
        slope[at, :] = logistic * (1.0 + pre * (1.0 - logistic))
        active = (pre * logistic).astype(bf16)
        active_out[at, :] = active
        branch = lax.dot_general(
            active, up_w, (((1,), (1,)), ((), ())), preferred_element_type=f32
        )
        residual = d[...].astype(f32) + branch * up_scale
        losses = losses + jnp.sum(residual * residual, axis=0, keepdims=True)
        upstream = (2.0 * residual).astype(bf16)
        upstream_out[at, :] = upstream
        part = jnp.dot(upstream, up_w, preferred_element_type=f32) * up_scale
        back[at, :] = part
        send[(1 - i) * block : (2 - i) * block, :] = part.astype(bf16)
    lane = lax.broadcasted_iota(jnp.int32, (1, 128), 1)
    tokens = own.shape[0] * (lax.axis_size("x") // 2) * lax.axis_size("z")
    mean = jnp.sum(losses, axis=1, keepdims=True) / (tokens * D)
    loss[...] = jnp.where(lane == 4 + particle_index(), mean, 0.0)


def parted(product, mine, theirs, full):
    own, other = halves()
    full[...] = product.reshape(full.shape)
    mine[...] = full[:, own]
    theirs[...] = full[:, other].astype(bf16)


def up_kernel(upstream, active, mine, theirs, full):
    turned = (((0,), (0,)), ((), ()))
    up = lax.dot_general(upstream[...], active[...], turned, preferred_element_type=f32)
    parted(up * up_scale, mine, theirs, full)


def back_kernel(own, received, slope, back):
    back[...] = ((own[...] + received[...].astype(f32)) * slope[...]).astype(bf16)


def last_kernel(back, received, n0, n1, n2, n3, up, up_in, terms):
    block = n0.shape[0]
    down = 0.0
    for n, source, i in ((n0, back, 0), (n1, back, 1), (n3, received, 0), (n2, received, 1)):
        down = down + lax.dot_general(
            n[...],
            source[i * block : (i + 1) * block, :],
            (((0,), (0,)), ((), ())),
            preferred_element_type=f32,
        )
    terms[:, 0] = (down * down_scale).astype(bf16).reshape(up.shape)
    terms[:, 1] = (up[...] + up_in[...].astype(f32)).astype(bf16)


def total_kernel(received, losses, gradient, line):
    full = losses[...]
    lane = lax.broadcasted_iota(jnp.int32, full.shape, 1) - 2 * lax.axis_index("core")
    for half in range(gradient.shape[0]):
        total = received[0, half].astype(f32)
        for i in range(1, received.shape[0]):
            total = total + received[i, half].astype(f32)
        gradient[half] = total
        square = jnp.sum(jnp.sum(total * total, axis=0, keepdims=True), axis=1, keepdims=True)
        full = full + jnp.where(lane == half, square, 0.0)
    line[...] = jnp.broadcast_to(full[None], line.shape)


def add_kernel(a, b, out):
    out[...] = a[...] + b[...]


def learned_kernel(base, perturbation, out):
    particle = particle_index()
    row = lax.broadcasted_iota(jnp.int32, perturbation.shape, 0)
    own = jnp.sum(
        jnp.where(row == particle // 2, perturbation[...], 0.0), axis=0, keepdims=True
    )
    out[...] = base[...] + jnp.where(lax.rem(particle, 2) == 0, own, -own)


def update_kernel(
    learned,
    sums,
    gradient,
    weights,
    first,
    second,
    accumulated,
    perturbation,
    new_weights,
    new_first,
    new_second,
    own_loss,
    outer,
):
    total = jnp.sum(sums[...], axis=0)
    lane = lax.broadcasted_iota(jnp.int32, total.shape, 1)
    elements = D * RANK
    mine = 2 * lax.axis_index("core")
    pairs = accumulated.shape[0]
    own_loss[...] = jnp.sum(jnp.where(lane == 4 + particle_index(), total, 0.0), axis=1, keepdims=True)
    row = lax.broadcasted_iota(jnp.int32, (pairs, total.shape[1]), 0)
    spot = lax.broadcasted_iota(jnp.int32, (pairs, total.shape[1]), 1)
    signs = jnp.where(spot == 4 + 2 * row, 1.0, 0.0) - jnp.where(spot == 5 + 2 * row, 1.0, 0.0)
    difference = jnp.sum(signs * total, axis=1, keepdims=True)
    outer[...] = jnp.sum(
        difference * (accumulated[...] + perturbation[...]), axis=0, keepdims=True
    ) / (2 * pairs)
    chunk = 32
    for half in range(2):
        square = jnp.sum(jnp.where(lane == mine + half, total, 0.0), axis=1, keepdims=True)
        factor = lax.rsqrt(square / elements + grad_eps)
        for start in range(0, weights.shape[1], chunk):
            at = (half, pl.ds(start, chunk))
            weight = weights[at]
            scaled = gradient[at] * factor
            m = beta_one * first[at] + (1.0 - beta_one) * scaled
            v = beta_two * second[at] + (1.0 - beta_two) * scaled * scaled
            new_first[at] = m
            new_second[at] = v
            inverse = lax.rsqrt(v)
            momentum = m * inverse
            speed = scaled * inverse
            out_a = jnp.zeros_like(momentum)
            out_b = jnp.zeros_like(momentum)
            for h in range(HIDDEN):
                act = jnp.tanh(
                    speed * learned[h]
                    + momentum * learned[HIDDEN + h]
                    + weight * learned[2 * HIDDEN + h]
                    + learned[3 * HIDDEN + h]
                )
                out_a = out_a + act * learned[4 * HIDDEN + h]
                out_b = out_b + act * learned[5 * HIDDEN + h]
            new_weights[at] = weight - step_size * (momentum + out_a) * jnp.exp(jnp.tanh(out_b))


def swap(array, axis, mask):
    pairs = [(i, i ^ mask) for i in range(lax.axis_size(axis))]
    return lax.ppermute(array, axis, pairs)


def exchange(array, axis):
    return lax.all_to_all(array, axis, 0, 0, tiled=True)


def plus(a, b):
    return call(add_kernel, [(a.shape, a.dtype)], (a, b), a.size)[0]


def local(
    tokens,
    targets,
    norm_gain,
    weights,
    first_moment,
    second_moment,
    learned_params,
    perturbation,
    accumulated,
):
    nz, nx = lax.axis_size("z"), lax.axis_size("x")
    rows = weights.shape[2]
    block = tokens.shape[0]
    width = 2 * nz * rows
    tall = 2 * block
    shape = (weights.shape[1], rows, RANK)
    column = (nz, rows, RANK)
    full = (nz, 2 * rows, RANK)
    up_size = nz * rows * RANK
    (copies,) = call(copies_kernel, [((nz, *shape), bf16)], (weights[0],), weights.size)
    gathered = exchange(copies, "z")
    cuts = call(
        cut_kernel,
        [((block, width // 2), bf16)] * nx + [((block, width), bf16)] * 2,
        (tokens, targets, norm_gain[None]),
        20 * block * D,
    )
    normed = [cuts[0]] + [swap(cuts[k], "x", k) for k in range(1, nx)]
    gaps = (cuts[nx], swap(cuts[nx + 1], "x", 1))
    (up_w,) = call(split_kernel, [(column, bf16)], (gathered,), up_size)
    up_w = (up_w, swap(up_w, "x", 3))

    wide, thin = ((tall, RANK), f32), ((tall, RANK), bf16)
    product = 2 * tall * width * RANK
    pre, *sends = call(first_kernel, [wide] + [thin] * 3, (*normed, gathered), product)
    sends = [swap(s, "x", k + 1) for k, s in enumerate(sends)]
    slope, active, upstream, loss, back, send = call(
        middle_kernel,
        [wide, thin, ((tall, width), bf16), ((1, 128), f32), wide, thin],
        (pre, *sends, *gaps, *up_w),
        2 * product,
        [(full, bf16)],
    )
    received = swap(send, "x", 1)
    parts = [(column, f32), (column, bf16)]
    up, send = call(up_kernel, parts, (upstream, active), product, [(full, f32)])
    up_in = swap(send, "x", 3)
    (back,) = call(back_kernel, [thin], (back, received, slope), 2 * back.size)
    back_in = swap(back, "x", 3)
    loss = plus(loss, swap(loss, "y", 1))
    back_in, loss = lax.optimization_barrier((back_in, loss))
    (terms,) = call(
        last_kernel, [((nz, *shape), bf16)], (back, back_in, *normed, up, up_in), product
    )
    terms = exchange(terms, "z")
    loss = plus(loss, swap(loss, "y", 2))
    loss = plus(loss, swap(loss, "y", 4))
    gradient, line = call(
        total_kernel,
        [(shape, f32), ((lax.axis_size("core") * nz * nx, 1, 128), f32)],
        (terms, loss),
        10 * terms.size,
    )
    sums = exchange(line, ("core", "z", "x"))
    (learned,) = call(
        learned_kernel,
        [((1, learned_params.shape[0]), f32)],
        (learned_params[None], perturbation),
        10 * perturbation.size,
    )
    learned = learned.reshape(-1)
    new_w, new_m, new_v, own_loss, outer = call(
        update_kernel,
        [(shape, f32)] * 3 + [((1, 1), f32), ((1, learned.shape[0]), f32)],
        (
            learned,
            sums,
            gradient,
            weights[0],
            first_moment[0],
            second_moment[0],
            accumulated,
            perturbation,
        ),
        400 * weights.size,
    )
    return (new_w[None], new_m[None], new_v[None], own_loss.reshape(1), outer.reshape(-1))


def solution(mesh):
    grid = Mesh(mesh.devices.reshape(8, 2, 8, 4), ("y", "core", "z", "x"))
    pop, shard = ("y", "core"), ("z", "x")
    return jax.shard_map(
        local,
        mesh=grid,
        in_specs=(
            P(shard, None),
            P(shard, None),
            P(),
            P(pop, None, shard, None),
            P(pop, None, shard, None),
            P(pop, None, shard, None),
            P(),
            P(),
            P(),
        ),
        out_specs=(
            P(pop, None, shard, None),
            P(pop, None, shard, None),
            P(pop, None, shard, None),
            P(pop),
            P(),
        ),
        check_vma=False,
    )
```

```python
import jax
import jax.numpy as jnp
from jax import lax
from jax.experimental import pallas as pl
from jax.experimental.pallas import tpu as pltpu
from jax.sharding import Mesh, PartitionSpec as P


D = 2048
RANK = 256
HIDDEN = 32

step_size = 0.1
beta_one = 0.9
beta_two = 0.99
norm_eps = 1e-05
grad_eps = 1e-06
down_scale = D ** (-0.5)
up_scale = RANK ** (-0.5)
f32 = jnp.float32
bf16 = jnp.bfloat16
VMEM = pl.BlockSpec(memory_space=pltpu.VMEM)
SMEM = pl.BlockSpec(memory_space=pltpu.SMEM)
ANY = pl.BlockSpec(memory_space=pl.ANY)


def call(kernel, outs, args, flops, scratch=(), copied=0, copies=0):
    scalars = [a.ndim == 1 for a in args]
    moved = sum(a.size * a.dtype.itemsize for a in args)
    return pl.pallas_call(
        kernel,
        out_shape=[jax.ShapeDtypeStruct(s, d) for s, d in outs],
        in_specs=[SMEM if s else VMEM for s in scalars],
        out_specs=[ANY] * copied + [VMEM] * (len(outs) - copied),
        scratch_shapes=[pltpu.VMEM(s, d) for s, d in scratch]
        + ([pltpu.SemaphoreType.DMA((copies,))] if copies else []),
        compiler_params=pltpu.CompilerParams(vmem_limit_bytes=16 * 2**20),
        cost_estimate=pl.CostEstimate(flops=flops, bytes_accessed=moved, transcendentals=0),
    )(*args)


def copies_kernel(weights, copies, rounded, sems):
    rounded[...] = weights[...].astype(bf16)
    moves = [
        pltpu.make_async_copy(rounded, copies.at[i], sems.at[i]) for i in range(copies.shape[0])
    ]
    for move in moves:
        move.start()
    for move in moves:
        move.wait()


def cut_kernel(tokens, targets, gain, *outs):
    tile = 128
    block, side = tokens.shape[0], tile // 2
    my_x = lax.axis_index("x")
    outer = my_x // 2 == lax.rem(my_x, 2)
    lanes = lax.broadcasted_iota(jnp.int32, (block, tile), 1) < side
    values = tokens[...].astype(f32)
    inverse = lax.rsqrt(jnp.mean(values * values, axis=-1, keepdims=True) + norm_eps)
    norms = []
    for q in range(tokens.shape[1] // (2 * tile)):
        pair, gaps = [], []
        for j in range(2):
            at = slice((2 * q + j) * tile, (2 * q + j + 1) * tile)
            token = tokens[:, at].astype(f32)
            pair.append(token * inverse * gain[:, at])
            gaps.append(token - targets[:, at].astype(f32))
        norms.append(pair)
        out = slice(q * tile, (q + 1) * tile)
        for k, dest in enumerate(outs[4:]):
            first = jnp.logical_xor(lanes, outer if k else jnp.logical_not(outer))
            dest[:, out] = jnp.where(first, *gaps).astype(bf16)
    for k, dest in enumerate(outs[:4]):
        x = jnp.bitwise_xor(my_x, k)
        high, odd = x // 2 == 1, lax.rem(x, 2) == 1
        keep = jnp.logical_xor(lanes, odd)
        for q in range(len(norms) // 2):
            a, b = (jnp.where(high, n[1], n[0]) for n in norms[2 * q : 2 * q + 2])
            moved = pltpu.roll(jnp.where(odd, a, b), side, 1)
            kept = jnp.where(odd, b, a)
            dest[:, q * tile : (q + 1) * tile] = jnp.where(keep, kept, moved).astype(bf16)


def halves():
    half = lax.rem(lax.axis_index("x"), 2)
    rows = 64
    return [pl.ds(pl.multiple_of(h * rows, rows), rows) for h in (half, 1 - half)]


def particle_index():
    return lax.axis_index("y") * lax.axis_size("core") + lax.axis_index("core")


def joined(mine, theirs, full):
    own, other = halves()
    full[:, own] = mine
    full[:, other] = theirs.reshape(mine.shape)
    return full[...].reshape(-1, full.shape[-1])


def first_kernel(n0, n1, n2, n3, gathered, own, s1, s2, s3):
    down_w = gathered[:, 0].reshape(-1, RANK)
    block = n0.shape[0]
    for i, n in enumerate((n0, n1, n2, n3)):
        part = jnp.dot(n[...], down_w, preferred_element_type=f32) * down_scale
        for k, dest in enumerate((own, s1, s2, s3)):
            j = i ^ k
            if j < 2:
                dest[j * block : (j + 1) * block, :] = part.astype(dest.dtype)
    s3[2 * block :, :] = gathered[:, 1].reshape(-1, RANK)


def middle_kernel(
    own, r1, r2, r3, d0, d1, gathered, slope, active_out, upstream_out, loss, back, send, full
):
    up_w = joined(gathered[:, 1], r3[own.shape[0] :, :], full)
    losses = 0.0
    block = d0.shape[0]
    for i, d in enumerate((d0, d1)):
        at = slice(i * block, (i + 1) * block)
        pre = (own[at, :] + r1[at, :].astype(f32)) + (r2[at, :].astype(f32) + r3[at, :].astype(f32))
        logistic = jax.nn.sigmoid(pre)
        slope[at, :] = logistic * (1.0 + pre * (1.0 - logistic))
        active = (pre * logistic).astype(bf16)
        active_out[at, :] = active
        branch = lax.dot_general(
            active, up_w, (((1,), (1,)), ((), ())), preferred_element_type=f32
        )
        residual = d[...].astype(f32) + branch * up_scale
        losses = losses + jnp.sum(residual * residual, axis=0, keepdims=True)
        upstream = (2.0 * residual).astype(bf16)
        upstream_out[at, :] = upstream
        part = jnp.dot(upstream, up_w, preferred_element_type=f32) * up_scale
        back[at, :] = part
        send[(1 - i) * block : (2 - i) * block, :] = part.astype(bf16)
    lane = lax.broadcasted_iota(jnp.int32, (1, 128), 1)
    tokens = own.shape[0] * (lax.axis_size("x") // 2) * lax.axis_size("z")
    mean = jnp.sum(losses, axis=1, keepdims=True) / (tokens * D)
    loss[...] = jnp.where(lane == 4 + particle_index(), mean, 0.0)


def parted(product, mine, theirs, full):
    own, other = halves()
    full[...] = product.reshape(full.shape)
    mine[...] = full[:, own]
    theirs[...] = full[:, other].astype(bf16)


def up_kernel(upstream, active, mine, theirs, full):
    turned = (((0,), (0,)), ((), ()))
    up = lax.dot_general(upstream[...], active[...], turned, preferred_element_type=f32)
    parted(up * up_scale, mine, theirs, full)


def back_kernel(own, received, slope, back):
    back[...] = ((own[...] + received[...].astype(f32)) * slope[...]).astype(bf16)


def last_kernel(back, received, n0, n1, n2, n3, up, up_in, terms, down_out, up_out, sems):
    moves = [
        pltpu.make_async_copy(source, terms.at[:, i], sems.at[i])
        for i, source in enumerate((down_out, up_out))
    ]
    up_out[...] = (up[...] + up_in[...].astype(f32)).astype(bf16)
    moves[1].start()
    block = n0.shape[0]
    down = 0.0
    for n, source, i in ((n0, back, 0), (n1, back, 1), (n3, received, 0), (n2, received, 1)):
        down = down + lax.dot_general(
            n[...],
            source[i * block : (i + 1) * block, :],
            (((0,), (0,)), ((), ())),
            preferred_element_type=f32,
        )
    down_out[...] = (down * down_scale).astype(bf16).reshape(up.shape)
    moves[0].start()
    moves[1].wait()
    moves[0].wait()


def total_kernel(received, losses, gradient, line):
    full = losses[...]
    lane = lax.broadcasted_iota(jnp.int32, full.shape, 1) - 2 * lax.axis_index("core")
    for half in range(gradient.shape[0]):
        total = received[0, half].astype(f32)
        for i in range(1, received.shape[0]):
            total = total + received[i, half].astype(f32)
        gradient[half] = total
        square = jnp.sum(jnp.sum(total * total, axis=0, keepdims=True), axis=1, keepdims=True)
        full = full + jnp.where(lane == half, square, 0.0)
    line[...] = jnp.broadcast_to(full[None], line.shape)


def add_kernel(a, b, out):
    out[...] = a[...] + b[...]


def learned_kernel(base, perturbation, out):
    particle = particle_index()
    row = lax.broadcasted_iota(jnp.int32, perturbation.shape, 0)
    own = jnp.sum(
        jnp.where(row == particle // 2, perturbation[...], 0.0), axis=0, keepdims=True
    )
    out[...] = base[...] + jnp.where(lax.rem(particle, 2) == 0, own, -own)


def update_kernel(
    learned,
    sums,
    gradient,
    weights,
    first,
    second,
    accumulated,
    perturbation,
    weights_out,
    first_out,
    second_out,
    own_loss,
    outer,
    new_weights,
    new_first,
    new_second,
    sems,
):
    total = jnp.sum(sums[...], axis=0)
    lane = lax.broadcasted_iota(jnp.int32, total.shape, 1)
    elements = D * RANK
    mine = 2 * lax.axis_index("core")
    pairs = accumulated.shape[0]
    own_loss[...] = jnp.sum(jnp.where(lane == 4 + particle_index(), total, 0.0), axis=1, keepdims=True)
    row = lax.broadcasted_iota(jnp.int32, (pairs, total.shape[1]), 0)
    spot = lax.broadcasted_iota(jnp.int32, (pairs, total.shape[1]), 1)
    signs = jnp.where(spot == 4 + 2 * row, 1.0, 0.0) - jnp.where(spot == 5 + 2 * row, 1.0, 0.0)
    difference = jnp.sum(signs * total, axis=1, keepdims=True)
    outer[...] = jnp.sum(
        difference * (accumulated[...] + perturbation[...]), axis=0, keepdims=True
    ) / (2 * pairs)
    chunk = 32
    buffers = (new_first, new_second, new_weights)
    moves = []
    for half in range(2):
        square = jnp.sum(jnp.where(lane == mine + half, total, 0.0), axis=1, keepdims=True)
        factor = lax.rsqrt(square / elements + grad_eps)
        for start in range(0, weights.shape[1], chunk):
            at = (half, pl.ds(start, chunk))
            weight = weights[at]
            scaled = gradient[at] * factor
            m = beta_one * first[at] + (1.0 - beta_one) * scaled
            v = beta_two * second[at] + (1.0 - beta_two) * scaled * scaled
            new_first[at] = m
            new_second[at] = v
            inverse = lax.rsqrt(v)
            momentum = m * inverse
            speed = scaled * inverse
            out_a = jnp.zeros_like(momentum)
            out_b = jnp.zeros_like(momentum)
            for h in range(HIDDEN):
                act = jnp.tanh(
                    speed * learned[h]
                    + momentum * learned[HIDDEN + h]
                    + weight * learned[2 * HIDDEN + h]
                    + learned[3 * HIDDEN + h]
                )
                out_a = out_a + act * learned[4 * HIDDEN + h]
                out_b = out_b + act * learned[5 * HIDDEN + h]
            new_weights[at] = weight - step_size * (momentum + out_a) * jnp.exp(jnp.tanh(out_b))
        for i, dest in enumerate((first_out, second_out, weights_out)):
            move = pltpu.make_async_copy(
                buffers[i].at[half], dest.at[half], sems.at[3 * half + i]
            )
            move.start()
            moves.append(move)
    for move in moves:
        move.wait()


def swap(array, axis, mask):
    pairs = [(i, i ^ mask) for i in range(lax.axis_size(axis))]
    return lax.ppermute(array, axis, pairs)


def exchange(array, axis):
    return lax.all_to_all(array, axis, 0, 0, tiled=True)


def plus(a, b):
    return call(add_kernel, [(a.shape, a.dtype)], (a, b), a.size)[0]


def local(
    tokens,
    targets,
    norm_gain,
    weights,
    first_moment,
    second_moment,
    learned_params,
    perturbation,
    accumulated,
):
    nz, nx = lax.axis_size("z"), lax.axis_size("x")
    rows = weights.shape[2]
    block = tokens.shape[0]
    width = 2 * nz * rows
    tall = 2 * block
    shape = (weights.shape[1], rows, RANK)
    column = (nz, rows, RANK)
    full = (nz, 2 * rows, RANK)
    (copies,) = call(
        copies_kernel, [((nz, *shape), bf16)], (weights[0],), weights.size, [(shape, bf16)], 1, nz
    )
    gathered = exchange(copies, "z")
    cuts = call(
        cut_kernel,
        [((block, width // 2), bf16)] * nx + [((block, width), bf16)] * 2,
        (tokens, targets, norm_gain[None]),
        20 * block * D,
    )
    normed = [cuts[0]] + [swap(cuts[k], "x", k) for k in range(1, nx)]
    gaps = (cuts[nx], swap(cuts[nx + 1], "x", 1))
    wide, thin = ((tall, RANK), f32), ((tall, RANK), bf16)
    product = 2 * tall * width * RANK
    pre, *sends = call(
        first_kernel,
        [wide, thin, thin, ((tall + nz * rows, RANK), bf16)],
        (*normed, gathered),
        product,
    )
    sends = [swap(s, "x", k + 1) for k, s in enumerate(sends)]
    slope, active, upstream, loss, back, send = call(
        middle_kernel,
        [wide, thin, ((tall, width), bf16), ((1, 128), f32), wide, thin],
        (pre, *sends, *gaps, gathered),
        2 * product,
        [(full, bf16)],
    )
    received = swap(send, "x", 1)
    parts = [(column, f32), (column, bf16)]
    up, send = call(up_kernel, parts, (upstream, active), product, [(full, f32)])
    up_in = swap(send, "x", 3)
    (back,) = call(back_kernel, [thin], (back, received, slope), 2 * back.size)
    back_in = swap(back, "x", 3)
    loss = plus(loss, swap(loss, "y", 1))
    back_in, loss = lax.optimization_barrier((back_in, loss))
    (terms,) = call(
        last_kernel,
        [((nz, *shape), bf16)],
        (back, back_in, *normed, up, up_in),
        product,
        [(column, bf16)] * 2,
        1,
        2,
    )
    terms = exchange(terms, "z")
    loss = plus(loss, swap(loss, "y", 2))
    loss = plus(loss, swap(loss, "y", 6))
    (learned,) = call(
        learned_kernel,
        [((1, learned_params.shape[0]), f32)],
        (learned_params[None], perturbation),
        10 * perturbation.size,
    )
    loss, learned = lax.optimization_barrier((loss, learned))
    learned = learned.reshape(-1)
    gradient, line = call(
        total_kernel,
        [(shape, f32), ((lax.axis_size("core") * nz * nx, 1, 128), f32)],
        (terms, loss),
        10 * terms.size,
    )
    sums = exchange(line, ("core", "z", "x"))
    new_w, new_m, new_v, own_loss, outer = call(
        update_kernel,
        [(shape, f32)] * 3 + [((1, 1), f32), ((1, learned.shape[0]), f32)],
        (
            learned,
            sums,
            gradient,
            weights[0],
            first_moment[0],
            second_moment[0],
            accumulated,
            perturbation,
        ),
        400 * weights.size,
        [(shape, f32)] * 3,
        3,
        6,
    )
    return (new_w[None], new_m[None], new_v[None], own_loss.reshape(1), outer.reshape(-1))


def solution(mesh):
    grid = Mesh(mesh.devices.reshape(8, 2, 8, 4), ("y", "core", "z", "x"))
    pop, shard = ("y", "core"), ("z", "x")
    return jax.shard_map(
        local,
        mesh=grid,
        in_specs=(
            P(shard, None),
            P(shard, None),
            P(),
            P(pop, None, shard, None),
            P(pop, None, shard, None),
            P(pop, None, shard, None),
            P(),
            P(),
            P(),
        ),
        out_specs=(
            P(pop, None, shard, None),
            P(pop, None, shard, None),
            P(pop, None, shard, None),
            P(pop),
            P(),
        ),
        check_vma=False,
    )
```

```python
import jax
import jax.numpy as jnp
from jax import lax
from jax.experimental import pallas as pl
from jax.experimental.pallas import tpu as pltpu
from jax.sharding import Mesh, PartitionSpec as P


D = 2048
RANK = 256
HIDDEN = 32

step_size = 0.1
beta_one = 0.9
beta_two = 0.99
norm_eps = 1e-05
grad_eps = 1e-06
down_scale = D ** (-0.5)
up_scale = RANK ** (-0.5)
f32 = jnp.float32
bf16 = jnp.bfloat16
VMEM = pl.BlockSpec(memory_space=pltpu.VMEM)
SMEM = pl.BlockSpec(memory_space=pltpu.SMEM)


def call(kernel, outs, args, flops, scratch=()):
    scalars = [a.ndim == 1 for a in args]
    moved = sum(a.size * a.dtype.itemsize for a in args)
    return pl.pallas_call(
        kernel,
        out_shape=[jax.ShapeDtypeStruct(s, d) for s, d in outs],
        in_specs=[SMEM if s else VMEM for s in scalars],
        out_specs=[VMEM] * len(outs),
        scratch_shapes=[pltpu.VMEM(s, d) for s, d in scratch],
        compiler_params=pltpu.CompilerParams(vmem_limit_bytes=16 * 2**20),
        cost_estimate=pl.CostEstimate(flops=flops, bytes_accessed=moved, transcendentals=0),
    )(*args)


def copies_kernel(weights, copies):
    for i in range(copies.shape[0]):
        copies[i] = weights[...].astype(bf16)


def cut_kernel(tokens, targets, gain, *outs):
    tile = 128
    block, side = tokens.shape[0], tile // 2
    my_x = lax.axis_index("x")
    outer = my_x // 2 == lax.rem(my_x, 2)
    lanes = lax.broadcasted_iota(jnp.int32, (block, tile), 1) < side
    values = tokens[...].astype(f32)
    inverse = lax.rsqrt(jnp.mean(values * values, axis=-1, keepdims=True) + norm_eps)
    norms = []
    for q in range(tokens.shape[1] // (2 * tile)):
        pair, gaps = [], []
        for j in range(2):
            at = slice((2 * q + j) * tile, (2 * q + j + 1) * tile)
            token = tokens[:, at].astype(f32)
            pair.append(token * inverse * gain[:, at])
            gaps.append(token - targets[:, at].astype(f32))
        norms.append(pair)
        out = slice(q * tile, (q + 1) * tile)
        for k, dest in enumerate(outs[4:]):
            first = jnp.logical_xor(lanes, outer if k else jnp.logical_not(outer))
            dest[:, out] = jnp.where(first, *gaps).astype(bf16)
    for k, dest in enumerate(outs[:4]):
        x = jnp.bitwise_xor(my_x, k)
        high, odd = x // 2 == 1, lax.rem(x, 2) == 1
        keep = jnp.logical_xor(lanes, odd)
        for q in range(len(norms) // 2):
            a, b = (jnp.where(high, n[1], n[0]) for n in norms[2 * q : 2 * q + 2])
            moved = pltpu.roll(jnp.where(odd, a, b), side, 1)
            kept = jnp.where(odd, b, a)
            dest[:, q * tile : (q + 1) * tile] = jnp.where(keep, kept, moved).astype(bf16)


def halves():
    half = lax.rem(lax.axis_index("x"), 2)
    rows = 64
    return [pl.ds(pl.multiple_of(h * rows, rows), rows) for h in (half, 1 - half)]


def particle_index():
    return lax.axis_index("y") * lax.axis_size("core") + lax.axis_index("core")


def joined(mine, theirs, full):
    own, other = halves()
    full[:, own] = mine
    full[:, other] = theirs.reshape(mine.shape)
    return full[...].reshape(-1, full.shape[-1])


def first_kernel(n0, n1, n2, n3, gathered, own, s1, s2, s3):
    down_w = gathered[:, 0].reshape(-1, RANK)
    block = n0.shape[0]
    for i, n in enumerate((n0, n1, n2, n3)):
        part = jnp.dot(n[...], down_w, preferred_element_type=f32) * down_scale
        for k, dest in enumerate((own, s1, s2, s3)):
            j = i ^ k
            if j < 2:
                dest[j * block : (j + 1) * block, :] = part.astype(dest.dtype)
    s3[2 * block :, :] = gathered[:, 1].reshape(-1, RANK)


def middle_kernel(
    own, r1, r2, r3, d0, d1, gathered, slope, active_out, upstream_out, loss, back, send, full
):
    up_w = joined(gathered[:, 1], r3[own.shape[0] :, :], full)
    losses = 0.0
    block = d0.shape[0]
    for i, d in enumerate((d0, d1)):
        at = slice(i * block, (i + 1) * block)
        pre = (own[at, :] + r1[at, :].astype(f32)) + (r2[at, :].astype(f32) + r3[at, :].astype(f32))
        logistic = jax.nn.sigmoid(pre)
        slope[at, :] = logistic * (1.0 + pre * (1.0 - logistic))
        active = (pre * logistic).astype(bf16)
        active_out[at, :] = active
        branch = lax.dot_general(
            active, up_w, (((1,), (1,)), ((), ())), preferred_element_type=f32
        )
        residual = d[...].astype(f32) + branch * up_scale
        losses = losses + jnp.sum(residual * residual, axis=0, keepdims=True)
        upstream = (2.0 * residual).astype(bf16)
        upstream_out[at, :] = upstream
        part = jnp.dot(upstream, up_w, preferred_element_type=f32) * up_scale
        back[at, :] = part
        send[(1 - i) * block : (2 - i) * block, :] = part.astype(bf16)
    lane = lax.broadcasted_iota(jnp.int32, (1, 128), 1)
    tokens = own.shape[0] * (lax.axis_size("x") // 2) * lax.axis_size("z")
    mean = jnp.sum(losses, axis=1, keepdims=True) / (tokens * D)
    loss[...] = jnp.where(lane == 4 + particle_index(), mean, 0.0)


def parted(product, mine, theirs, full):
    own, other = halves()
    full[...] = product.reshape(full.shape)
    mine[...] = full[:, own]
    theirs[...] = full[:, other].astype(bf16)


def up_kernel(upstream, active, mine, theirs, full):
    turned = (((0,), (0,)), ((), ()))
    up = lax.dot_general(upstream[...], active[...], turned, preferred_element_type=f32)
    parted(up * up_scale, mine, theirs, full)


def back_kernel(own, received, slope, back):
    back[...] = ((own[...] + received[...].astype(f32)) * slope[...]).astype(bf16)


def last_kernel(back, received, n0, n1, n2, n3, up, up_in, terms):
    block = n0.shape[0]
    down = 0.0
    for n, source, i in ((n0, back, 0), (n1, back, 1), (n3, received, 0), (n2, received, 1)):
        down = down + lax.dot_general(
            n[...],
            source[i * block : (i + 1) * block, :],
            (((0,), (0,)), ((), ())),
            preferred_element_type=f32,
        )
    terms[:, 0] = (down * down_scale).astype(bf16).reshape(up.shape)
    terms[:, 1] = (up[...] + up_in[...].astype(f32)).astype(bf16)


def total_kernel(received, losses, gradient, line):
    full = losses[...]
    lane = lax.broadcasted_iota(jnp.int32, full.shape, 1) - 2 * lax.axis_index("core")
    for half in range(gradient.shape[0]):
        total = received[0, half].astype(f32)
        for i in range(1, received.shape[0]):
            total = total + received[i, half].astype(f32)
        gradient[half] = total
        square = jnp.sum(jnp.sum(total * total, axis=0, keepdims=True), axis=1, keepdims=True)
        full = full + jnp.where(lane == half, square, 0.0)
    line[...] = jnp.broadcast_to(full[None], line.shape)


def add_kernel(a, b, out):
    out[...] = a[...] + b[...]


def learned_kernel(base, perturbation, out):
    particle = particle_index()
    row = lax.broadcasted_iota(jnp.int32, perturbation.shape, 0)
    own = jnp.sum(
        jnp.where(row == particle // 2, perturbation[...], 0.0), axis=0, keepdims=True
    )
    out[...] = base[...] + jnp.where(lax.rem(particle, 2) == 0, own, -own)


def update_kernel(
    learned,
    sums,
    gradient,
    weights,
    first,
    second,
    accumulated,
    perturbation,
    new_weights,
    new_first,
    new_second,
    own_loss,
    outer,
):
    total = jnp.sum(sums[...], axis=0)
    lane = lax.broadcasted_iota(jnp.int32, total.shape, 1)
    elements = D * RANK
    mine = 2 * lax.axis_index("core")
    pairs = accumulated.shape[0]
    own_loss[...] = jnp.sum(jnp.where(lane == 4 + particle_index(), total, 0.0), axis=1, keepdims=True)
    row = lax.broadcasted_iota(jnp.int32, (pairs, total.shape[1]), 0)
    spot = lax.broadcasted_iota(jnp.int32, (pairs, total.shape[1]), 1)
    signs = jnp.where(spot == 4 + 2 * row, 1.0, 0.0) - jnp.where(spot == 5 + 2 * row, 1.0, 0.0)
    difference = jnp.sum(signs * total, axis=1, keepdims=True)
    outer[...] = jnp.sum(
        difference * (accumulated[...] + perturbation[...]), axis=0, keepdims=True
    ) / (2 * pairs)
    chunk = 32
    for half in range(2):
        square = jnp.sum(jnp.where(lane == mine + half, total, 0.0), axis=1, keepdims=True)
        factor = lax.rsqrt(square / elements + grad_eps)
        for start in range(0, weights.shape[1], chunk):
            at = (half, pl.ds(start, chunk))
            weight = weights[at]
            scaled = gradient[at] * factor
            m = beta_one * first[at] + (1.0 - beta_one) * scaled
            v = beta_two * second[at] + (1.0 - beta_two) * scaled * scaled
            new_first[at] = m
            new_second[at] = v
            inverse = lax.rsqrt(v)
            momentum = m * inverse
            speed = scaled * inverse
            out_a = jnp.zeros_like(momentum)
            out_b = jnp.zeros_like(momentum)
            for h in range(HIDDEN):
                act = jnp.tanh(
                    speed * learned[h]
                    + momentum * learned[HIDDEN + h]
                    + weight * learned[2 * HIDDEN + h]
                    + learned[3 * HIDDEN + h]
                )
                out_a = out_a + act * learned[4 * HIDDEN + h]
                out_b = out_b + act * learned[5 * HIDDEN + h]
            new_weights[at] = weight - step_size * (momentum + out_a) * jnp.exp(jnp.tanh(out_b))


def swap(array, axis, mask):
    pairs = [(i, i ^ mask) for i in range(lax.axis_size(axis))]
    return lax.ppermute(array, axis, pairs)


def exchange(array, axis):
    return lax.all_to_all(array, axis, 0, 0, tiled=True)


def plus(a, b):
    return call(add_kernel, [(a.shape, a.dtype)], (a, b), a.size)[0]


def local(
    tokens,
    targets,
    norm_gain,
    weights,
    first_moment,
    second_moment,
    learned_params,
    perturbation,
    accumulated,
):
    nz, nx = lax.axis_size("z"), lax.axis_size("x")
    rows = weights.shape[2]
    block = tokens.shape[0]
    width = 2 * nz * rows
    tall = 2 * block
    shape = (weights.shape[1], rows, RANK)
    column = (nz, rows, RANK)
    full = (nz, 2 * rows, RANK)
    (copies,) = call(copies_kernel, [((nz, *shape), bf16)], (weights[0],), weights.size)
    gathered = exchange(copies, "z")
    cuts = call(
        cut_kernel,
        [((block, width // 2), bf16)] * nx + [((block, width), bf16)] * 2,
        (tokens, targets, norm_gain[None]),
        20 * block * D,
    )
    normed = [cuts[0]] + [swap(cuts[k], "x", k) for k in range(1, nx)]
    gaps = (cuts[nx], swap(cuts[nx + 1], "x", 1))
    wide, thin = ((tall, RANK), f32), ((tall, RANK), bf16)
    product = 2 * tall * width * RANK
    pre, *sends = call(
        first_kernel,
        [wide, thin, thin, ((tall + nz * rows, RANK), bf16)],
        (*normed, gathered),
        product,
    )
    sends = [swap(s, "x", k + 1) for k, s in enumerate(sends)]
    slope, active, upstream, loss, back, send = call(
        middle_kernel,
        [wide, thin, ((tall, width), bf16), ((1, 128), f32), wide, thin],
        (pre, *sends, *gaps, gathered),
        2 * product,
        [(full, bf16)],
    )
    received = swap(send, "x", 1)
    parts = [(column, f32), (column, bf16)]
    up, send = call(up_kernel, parts, (upstream, active), product, [(full, f32)])
    up_in = swap(send, "x", 3)
    (back,) = call(back_kernel, [thin], (back, received, slope), 2 * back.size)
    back_in = swap(back, "x", 3)
    loss = plus(loss, swap(loss, "y", 1))
    back_in, loss = lax.optimization_barrier((back_in, loss))
    (terms,) = call(
        last_kernel, [((nz, *shape), bf16)], (back, back_in, *normed, up, up_in), product
    )
    terms = exchange(terms, "z")
    loss = plus(loss, swap(loss, "y", 2))
    loss = plus(loss, swap(loss, "y", 6))
    (learned,) = call(
        learned_kernel,
        [((1, learned_params.shape[0]), f32)],
        (learned_params[None], perturbation),
        10 * perturbation.size,
    )
    loss, learned = lax.optimization_barrier((loss, learned))
    learned = learned.reshape(-1)
    gradient, line = call(
        total_kernel,
        [(shape, f32), ((lax.axis_size("core") * nz * nx, 1, 128), f32)],
        (terms, loss),
        10 * terms.size,
    )
    sums = exchange(line, ("core", "z", "x"))
    new_w, new_m, new_v, own_loss, outer = call(
        update_kernel,
        [(shape, f32)] * 3 + [((1, 1), f32), ((1, learned.shape[0]), f32)],
        (
            learned,
            sums,
            gradient,
            weights[0],
            first_moment[0],
            second_moment[0],
            accumulated,
            perturbation,
        ),
        400 * weights.size,
    )
    return (new_w[None], new_m[None], new_v[None], own_loss.reshape(1), outer.reshape(-1))


def solution(mesh):
    grid = Mesh(mesh.devices.reshape(8, 2, 8, 4), ("y", "core", "z", "x"))
    pop, shard = ("y", "core"), ("z", "x")
    return jax.shard_map(
        local,
        mesh=grid,
        in_specs=(
            P(shard, None),
            P(shard, None),
            P(),
            P(pop, None, shard, None),
            P(pop, None, shard, None),
            P(pop, None, shard, None),
            P(),
            P(),
            P(),
        ),
        out_specs=(
            P(pop, None, shard, None),
            P(pop, None, shard, None),
            P(pop, None, shard, None),
            P(pop),
            P(),
        ),
        check_vma=False,
    )
```

```python
import jax
import jax.numpy as jnp
from jax import lax
from jax.experimental import pallas as pl
from jax.experimental.pallas import tpu as pltpu
from jax.sharding import Mesh, PartitionSpec as P


D = 2048
RANK = 256
HIDDEN = 32

step_size = 0.1
beta_one = 0.9
beta_two = 0.99
norm_eps = 1e-05
grad_eps = 1e-06
down_scale = D ** (-0.5)
up_scale = RANK ** (-0.5)
f32 = jnp.float32
bf16 = jnp.bfloat16
VMEM = pl.BlockSpec(memory_space=pltpu.VMEM)
SMEM = pl.BlockSpec(memory_space=pltpu.SMEM)


def call(kernel, outs, args, flops, scratch=()):
    scalars = [a.ndim == 1 for a in args]
    moved = sum(a.size * a.dtype.itemsize for a in args)
    return pl.pallas_call(
        kernel,
        out_shape=[jax.ShapeDtypeStruct(s, d) for s, d in outs],
        in_specs=[SMEM if s else VMEM for s in scalars],
        out_specs=[VMEM] * len(outs),
        scratch_shapes=[pltpu.VMEM(s, d) for s, d in scratch],
        compiler_params=pltpu.CompilerParams(vmem_limit_bytes=16 * 2**20),
        cost_estimate=pl.CostEstimate(flops=flops, bytes_accessed=moved, transcendentals=0),
    )(*args)


def copies_kernel(weights, copies):
    for i in range(copies.shape[0]):
        copies[i] = weights[...].astype(bf16)


def cut_kernel(tokens, targets, gain, *outs):
    tile = 128
    block, side = tokens.shape[0], tile // 2
    my_x = lax.axis_index("x")
    outer = my_x // 2 == lax.rem(my_x, 2)
    lanes = lax.broadcasted_iota(jnp.int32, (block, tile), 1) < side
    values = tokens[...].astype(f32)
    inverse = lax.rsqrt(jnp.mean(values * values, axis=-1, keepdims=True) + norm_eps)
    norms = []
    for q in range(tokens.shape[1] // (2 * tile)):
        pair, gaps = [], []
        for j in range(2):
            at = slice((2 * q + j) * tile, (2 * q + j + 1) * tile)
            token = tokens[:, at].astype(f32)
            pair.append(token * inverse * gain[:, at])
            gaps.append(token - targets[:, at].astype(f32))
        norms.append(pair)
        out = slice(q * tile, (q + 1) * tile)
        for k, dest in enumerate(outs[4:]):
            first = jnp.logical_xor(lanes, outer if k else jnp.logical_not(outer))
            dest[:, out] = jnp.where(first, *gaps).astype(bf16)
    for k, dest in enumerate(outs[:4]):
        x = jnp.bitwise_xor(my_x, k)
        high, odd = x // 2 == 1, lax.rem(x, 2) == 1
        keep = jnp.logical_xor(lanes, odd)
        for q in range(len(norms) // 2):
            a, b = (jnp.where(high, n[1], n[0]) for n in norms[2 * q : 2 * q + 2])
            moved = pltpu.roll(jnp.where(odd, a, b), side, 1)
            kept = jnp.where(odd, b, a)
            dest[:, q * tile : (q + 1) * tile] = jnp.where(keep, kept, moved).astype(bf16)


def halves():
    half = lax.rem(lax.axis_index("x"), 2)
    rows = 64
    return [pl.ds(pl.multiple_of(h * rows, rows), rows) for h in (half, 1 - half)]


def particle_index():
    y = lax.axis_index("y_high") * lax.axis_size("y_low") + lax.axis_index("y_low")
    return y * lax.axis_size("core") + lax.axis_index("core")


def joined(mine, theirs, full):
    own, other = halves()
    full[:, own] = mine
    full[:, other] = theirs.reshape(mine.shape)
    return full[...].reshape(-1, full.shape[-1])


def first_kernel(n0, n1, n2, n3, gathered, own, s1, s2, s3):
    down_w = gathered[:, 0].reshape(-1, RANK)
    block = n0.shape[0]
    for i, n in enumerate((n0, n1, n2, n3)):
        part = jnp.dot(n[...], down_w, preferred_element_type=f32) * down_scale
        for k, dest in enumerate((own, s1, s2, s3)):
            j = i ^ k
            if j < 2:
                dest[j * block : (j + 1) * block, :] = part.astype(dest.dtype)
    s3[2 * block :, :] = gathered[:, 1].reshape(-1, RANK)


def middle_kernel(
    own, r1, r2, r3, d0, d1, gathered, slope, active_out, upstream_out, loss, back, send, full
):
    up_w = joined(gathered[:, 1], r3[own.shape[0] :, :], full)
    losses = 0.0
    block = d0.shape[0]
    for i, d in enumerate((d0, d1)):
        at = slice(i * block, (i + 1) * block)
        pre = (own[at, :] + r1[at, :].astype(f32)) + (r2[at, :].astype(f32) + r3[at, :].astype(f32))
        logistic = jax.nn.sigmoid(pre)
        slope[at, :] = logistic * (1.0 + pre * (1.0 - logistic))
        active = (pre * logistic).astype(bf16)
        active_out[at, :] = active
        branch = lax.dot_general(
            active, up_w, (((1,), (1,)), ((), ())), preferred_element_type=f32
        )
        residual = d[...].astype(f32) + branch * up_scale
        losses = losses + jnp.sum(residual * residual, axis=0, keepdims=True)
        upstream = (2.0 * residual).astype(bf16)
        upstream_out[at, :] = upstream
        part = jnp.dot(upstream, up_w, preferred_element_type=f32) * up_scale
        back[at, :] = part
        send[(1 - i) * block : (2 - i) * block, :] = part.astype(bf16)
    lane = lax.broadcasted_iota(jnp.int32, (1, 128), 1)
    tokens = own.shape[0] * (lax.axis_size("x") // 2) * lax.axis_size("z")
    mean = jnp.sum(losses, axis=1, keepdims=True) / (tokens * D)
    loss[...] = jnp.where(lane == 4 + particle_index(), mean, 0.0)


def parted(product, mine, theirs, full):
    own, other = halves()
    full[...] = product.reshape(full.shape)
    mine[...] = full[:, own]
    theirs[...] = full[:, other].astype(bf16)


def up_kernel(upstream, active, mine, theirs, full):
    turned = (((0,), (0,)), ((), ()))
    up = lax.dot_general(upstream[...], active[...], turned, preferred_element_type=f32)
    parted(up * up_scale, mine, theirs, full)


def back_kernel(own, received, slope, back):
    back[...] = ((own[...] + received[...].astype(f32)) * slope[...]).astype(bf16)


def last_kernel(back, received, n0, n1, n2, n3, up, up_in, terms):
    block = n0.shape[0]
    down = 0.0
    for n, source, i in ((n0, back, 0), (n1, back, 1), (n3, received, 0), (n2, received, 1)):
        down = down + lax.dot_general(
            n[...],
            source[i * block : (i + 1) * block, :],
            (((0,), (0,)), ((), ())),
            preferred_element_type=f32,
        )
    terms[:, 0] = (down * down_scale).astype(bf16).reshape(up.shape)
    terms[:, 1] = (up[...] + up_in[...].astype(f32)).astype(bf16)


def total_kernel(received, losses, gradient, line):
    full = losses[...]
    lane = lax.broadcasted_iota(jnp.int32, full.shape, 1) - 2 * lax.axis_index("y_low")
    for half in range(gradient.shape[0]):
        total = received[0, half].astype(f32)
        for i in range(1, received.shape[0]):
            total = total + received[i, half].astype(f32)
        gradient[half] = total
        square = jnp.sum(jnp.sum(total * total, axis=0, keepdims=True), axis=1, keepdims=True)
        full = full + jnp.where(lane == half, square, 0.0)
    line[...] = jnp.broadcast_to(full[None], line.shape)


def add_kernel(a, b, out):
    out[...] = a[...] + b[...]


def learned_kernel(base, perturbation, out):
    particle = particle_index()
    row = lax.broadcasted_iota(jnp.int32, perturbation.shape, 0)
    own = jnp.sum(
        jnp.where(row == particle // 2, perturbation[...], 0.0), axis=0, keepdims=True
    )
    out[...] = base[...] + jnp.where(lax.rem(particle, 2) == 0, own, -own)


def update_kernel(
    learned,
    sums,
    gradient,
    weights,
    first,
    second,
    accumulated,
    perturbation,
    new_weights,
    new_first,
    new_second,
    own_loss,
    outer,
):
    total = jnp.sum(sums[...], axis=0)
    lane = lax.broadcasted_iota(jnp.int32, total.shape, 1)
    elements = D * RANK
    mine = 2 * lax.axis_index("y_low")
    pairs = accumulated.shape[0]
    own_loss[...] = jnp.sum(jnp.where(lane == 4 + particle_index(), total, 0.0), axis=1, keepdims=True)
    row = lax.broadcasted_iota(jnp.int32, (pairs, total.shape[1]), 0)
    spot = lax.broadcasted_iota(jnp.int32, (pairs, total.shape[1]), 1)
    signs = jnp.where(spot == 4 + 2 * row, 1.0, 0.0) - jnp.where(spot == 5 + 2 * row, 1.0, 0.0)
    difference = jnp.sum(signs * total, axis=1, keepdims=True)
    outer[...] = jnp.sum(
        difference * (accumulated[...] + perturbation[...]), axis=0, keepdims=True
    ) / (2 * pairs)
    chunk = 32
    for half in range(2):
        square = jnp.sum(jnp.where(lane == mine + half, total, 0.0), axis=1, keepdims=True)
        factor = lax.rsqrt(square / elements + grad_eps)
        for start in range(0, weights.shape[1], chunk):
            at = (half, pl.ds(start, chunk))
            weight = weights[at]
            scaled = gradient[at] * factor
            m = beta_one * first[at] + (1.0 - beta_one) * scaled
            v = beta_two * second[at] + (1.0 - beta_two) * scaled * scaled
            new_first[at] = m
            new_second[at] = v
            inverse = lax.rsqrt(v)
            momentum = m * inverse
            speed = scaled * inverse
            out_a = jnp.zeros_like(momentum)
            out_b = jnp.zeros_like(momentum)
            for h in range(HIDDEN):
                act = jnp.tanh(
                    speed * learned[h]
                    + momentum * learned[HIDDEN + h]
                    + weight * learned[2 * HIDDEN + h]
                    + learned[3 * HIDDEN + h]
                )
                out_a = out_a + act * learned[4 * HIDDEN + h]
                out_b = out_b + act * learned[5 * HIDDEN + h]
            new_weights[at] = weight - step_size * (momentum + out_a) * jnp.exp(jnp.tanh(out_b))


def swap(array, axis, mask):
    pairs = [(i, i ^ mask) for i in range(lax.axis_size(axis))]
    return lax.ppermute(array, axis, pairs)


def exchange(array, axis):
    return lax.all_to_all(array, axis, 0, 0, tiled=True)


def plus(a, b):
    return call(add_kernel, [(a.shape, a.dtype)], (a, b), a.size)[0]


def local(
    tokens,
    targets,
    norm_gain,
    weights,
    first_moment,
    second_moment,
    learned_params,
    perturbation,
    accumulated,
):
    nz, nx = lax.axis_size("z"), lax.axis_size("x")
    rows = weights.shape[2]
    block = tokens.shape[0]
    width = 2 * nz * rows
    tall = 2 * block
    shape = (weights.shape[1], rows, RANK)
    column = (nz, rows, RANK)
    full = (nz, 2 * rows, RANK)
    (copies,) = call(copies_kernel, [((nz, *shape), bf16)], (weights[0],), weights.size)
    gathered = exchange(copies, "z")
    cuts = call(
        cut_kernel,
        [((block, width // 2), bf16)] * nx + [((block, width), bf16)] * 2,
        (tokens, targets, norm_gain[None]),
        20 * block * D,
    )
    normed = [cuts[0]] + [swap(cuts[k], "x", k) for k in range(1, nx)]
    gaps = (cuts[nx], swap(cuts[nx + 1], "x", 1))
    wide, thin = ((tall, RANK), f32), ((tall, RANK), bf16)
    product = 2 * tall * width * RANK
    pre, *sends = call(
        first_kernel,
        [wide, thin, thin, ((tall + nz * rows, RANK), bf16)],
        (*normed, gathered),
        product,
    )
    sends = [swap(s, "x", k + 1) for k, s in enumerate(sends)]
    slope, active, upstream, loss, back, send = call(
        middle_kernel,
        [wide, thin, ((tall, width), bf16), ((1, 128), f32), wide, thin],
        (pre, *sends, *gaps, gathered),
        2 * product,
        [(full, bf16)],
    )
    received = swap(send, "x", 1)
    parts = [(column, f32), (column, bf16)]
    up, send = call(up_kernel, parts, (upstream, active), product, [(full, f32)])
    up_in = swap(send, "x", 3)
    (back,) = call(back_kernel, [thin], (back, received, slope), 2 * back.size)
    back_in = swap(back, "x", 3)
    loss = plus(loss, swap(loss, "core", 1))
    back_in, loss = lax.optimization_barrier((back_in, loss))
    (terms,) = call(
        last_kernel, [((nz, *shape), bf16)], (back, back_in, *normed, up, up_in), product
    )
    terms = exchange(terms, "z")
    loss = plus(loss, swap(loss, "y_high", 1))
    loss = plus(loss, swap(loss, "y_high", 3))
    (learned,) = call(
        learned_kernel,
        [((1, learned_params.shape[0]), f32)],
        (learned_params[None], perturbation),
        10 * perturbation.size,
    )
    loss, learned = lax.optimization_barrier((loss, learned))
    learned = learned.reshape(-1)
    gradient, line = call(
        total_kernel,
        [(shape, f32), ((lax.axis_size("y_low") * nz * nx, 1, 128), f32)],
        (terms, loss),
        10 * terms.size,
    )
    sums = exchange(line, ("y_low", "z", "x"))
    new_w, new_m, new_v, own_loss, outer = call(
        update_kernel,
        [(shape, f32)] * 3 + [((1, 1), f32), ((1, learned.shape[0]), f32)],
        (
            learned,
            sums,
            gradient,
            weights[0],
            first_moment[0],
            second_moment[0],
            accumulated,
            perturbation,
        ),
        400 * weights.size,
    )
    return (new_w[None], new_m[None], new_v[None], own_loss.reshape(1), outer.reshape(-1))


def solution(mesh):
    grid = Mesh(mesh.devices.reshape(4, 2, 2, 8, 4), ("y_high", "y_low", "core", "z", "x"))
    pop, shard = ("y_high", "y_low", "core"), ("z", "x")
    return jax.shard_map(
        local,
        mesh=grid,
        in_specs=(
            P(shard, None),
            P(shard, None),
            P(),
            P(pop, None, shard, None),
            P(pop, None, shard, None),
            P(pop, None, shard, None),
            P(),
            P(),
            P(),
        ),
        out_specs=(
            P(pop, None, shard, None),
            P(pop, None, shard, None),
            P(pop, None, shard, None),
            P(pop),
            P(),
        ),
        check_vma=False,
    )
```
